128 devices in a mesh: leaf: 128 (over z, y, x, core).
Axes of the slice: x: 4, y: 4, z: 4, core: 2. Of those that a mesh axis runs over, the one named last changes fastest.
Arguments:
- points: float32 [524288, 128], P('leaf')
- right_side: float32 [64, 524288], P(None, 'leaf'), may hold values from -6 to 6
- neighbours: int32 [1024, 5], P('leaf'), may hold values from -1 to 1023, as said below
- leaf_interp: float32 [1024, 512, 256], P('leaf'), may hold values from -0.25 to 0.25
- leaf_skeleton: int32 [1024, 256], P('leaf'), may hold values from 0 to 511, as said below
- node_skeleton: int32 [1022, 256], replicated, may hold values from 0 to 511, as said below
- node_gain: float32 [2046, 256], replicated, may hold values from 0.5 to 1.5
- transfer: float32 [9, 2, 256, 256], replicated, may hold values from -0.1875 to 0.1875
Outputs:
- solution: float32 [64, 524288], P(None, 'leaf')
- residual: float32 [64, 524288], P(None, 'leaf')
The draws below stay inside these ranges and needn't reach their ends.
Inputs may be any that keep to these rules, and one draw needn't show every extreme that they name: `neighbours`: slot s of leaf j holds j + s - 2 or -1, and slot 2 holds j; leaf m stands in leaf j's list exactly when j stands in leaf m's. `leaf_skeleton`: the entries of a row are distinct. `node_skeleton`: the entries of a row are distinct.
All inputs are finite; a program needn't handle non-finite values.
Results may differ from the reference program's by a relative error of at most 0.0003.
Values sent between devices are 32-bit elements; how exact they have to be, the bound alone decides.
A program may use at most 192 MiB of HBM per device.

```python
import math
import jax
import jax.numpy as jnp
from jax import lax

LEAF = 512
SKEL = 256
DIM = 128
CLASSES = 64
RANGE = 2
ITERS = 2
LEVELS = 10
LEAVES = 1024
POINTS = 524288


latent_dims = 8


def draw_points(key, part):
    embedding = jax.random.normal(jax.random.fold_in(key, 3000), (latent_dims, DIM), jnp.float32) * DIM ** (-0.5)
    centres = jnp.zeros((LEAVES, latent_dims), jnp.float32)
    for level in range(LEVELS + 1):
        offsets = jax.random.normal(jax.random.fold_in(key, level + 1), (LEAVES >> level, latent_dims), jnp.float32)
        centres = centres + 0.15 * jnp.repeat(offsets, 2 ** level, axis=0)
    radius = jnp.exp(jax.random.uniform(jax.random.fold_in(key, 1000), (LEAVES, LEAF, 1), jnp.float32, jnp.log(0.6), 0.0))
    latent = jax.random.normal(jax.random.fold_in(key, 2000), (LEAVES, LEAF, latent_dims), jnp.float32)
    located = centres[:, None, :] + radius * latent
    embedded = jnp.einsum('nqk,kd->nqd', located, embedding, precision=lax.Precision.HIGHEST)
    ambient = jax.random.normal(jax.random.fold_in(key, 4000), (LEAVES, LEAF, DIM), jnp.float32) * DIM ** (-0.5)
    return (embedded + ambient).reshape(POINTS, DIM)


def draw_neighbours(key, part):
    leaf_ids = jnp.arange(LEAVES, dtype=jnp.int32)
    links = jax.random.randint(key, (LEAVES, RANGE), 0, 4) > 0
    columns = []
    for offset in range(RANGE, 0, -1):
        lower = leaf_ids - offset
        linked = jnp.roll(links[:, offset - 1], offset) & (lower >= 0)
        columns.append(jnp.where(linked, lower, -1))
    columns.append(leaf_ids)
    for offset in range(1, RANGE + 1):
        upper = leaf_ids + offset
        linked = links[:, offset - 1] & (upper < LEAVES)
        columns.append(jnp.where(linked, upper, -1))
    return jnp.stack(columns, axis=1).astype(jnp.int32)


def distinct_rows(key, row_count, width, chosen):
    scores = jax.random.randint(key, (row_count, width), 0, 1 << 20) * width + jnp.arange(width, dtype=jnp.int32)[None, :]
    order = jnp.argsort(scores, axis=1)
    return order[:, :chosen].astype(jnp.int32)


def draw_leaf_skeleton(key, part):
    return distinct_rows(jax.random.fold_in(key, 11), LEAVES, LEAF, SKEL)


def draw_node_skeleton(key, part):
    return distinct_rows(jax.random.fold_in(key, 12), LEAVES - 2, 2 * SKEL, SKEL)


def block_levels(own_key, extent, cuts, smallest, largest):
    def one(dim, blocks):
        steps = jax.random.uniform(jax.random.fold_in(jax.random.fold_in(own_key, 6), dim), (blocks,), jnp.float32, smallest / len(cuts), largest / len(cuts))
        return jnp.repeat(jnp.exp(steps), extent[dim] // blocks).reshape((-1,) + (1,) * (len(extent) - dim - 1))

    loudness = one(*cuts[0])
    for cut in cuts[1:]:
        loudness = loudness * one(*cut)
    return loudness


def noise(key, shape, deviation, bound, cuts=(), kind=jnp.bfloat16):
    gain = block_levels(key, shape, cuts, -0.22, 0.18) if cuts else 1.0
    entries = jax.random.normal(key, shape, jnp.float32) * deviation * gain
    return jnp.minimum(jnp.maximum(entries, -bound), bound).astype(kind)


def setup_inputs(seed: int = 0) -> dict:
    arg_keys = jax.random.split(jax.random.key(seed), 9)
    points = draw_points(jax.random.fold_in(arg_keys[8], 71), 0)
    right_side = noise(arg_keys[1], (CLASSES, POINTS), 1.0, 6.0, ((1, 128),), jnp.float32)
    neighbours = draw_neighbours(jax.random.fold_in(arg_keys[8], 71), 0)
    leaf_interp = noise(arg_keys[3], (LEAVES, LEAF, SKEL), LEAF ** -0.5, 0.25, ((0, 128),), jnp.float32)
    leaf_skeleton = draw_leaf_skeleton(jax.random.fold_in(arg_keys[8], 71), 0)
    node_skeleton = draw_node_skeleton(jax.random.fold_in(arg_keys[8], 71), 0)
    node_gain = jnp.clip(jnp.exp(jax.random.uniform(arg_keys[6], (2 * LEAVES - 2, SKEL), jnp.float32, math.log(0.5), math.log(1.5))), 0.5, 1.5)
    transfer = noise(arg_keys[7], (LEVELS - 1, 2, SKEL, SKEL), (4 * SKEL) ** -0.5, 0.1875, (), jnp.float32)
    return {"points": points, "right_side": right_side, "neighbours": neighbours, "leaf_interp": leaf_interp, "leaf_skeleton": leaf_skeleton, "node_skeleton": node_skeleton, "node_gain": node_gain, "transfer": transfer}


highest = lax.Precision.HIGHEST
ridge = 1.0

def pair_kernel(first_set, second_set):
    inner = jnp.einsum('nqd,npd->nqp', first_set, second_set, precision=highest)
    first_norm = jnp.sum(first_set * first_set, axis=-1)
    second_norm = jnp.sum(second_set * second_set, axis=-1)
    return jnp.exp((2.0 * inner - first_norm[:, :, None] - second_norm[:, None, :]) * 0.5)

def symmetric(matrix):
    return 0.5 * (matrix + matrix.T)

def chol_apply(matrix, target):
    factor = jnp.linalg.cholesky(matrix)
    return jax.scipy.linalg.cho_solve((factor, True), target)

def reference(points, right_side, neighbours, leaf_interp, leaf_skeleton, node_skeleton, node_gain, transfer):
    coords = points.reshape(LEAVES, LEAF, DIM)
    near_mask = (neighbours >= 0).astype(jnp.float32)
    padded_coords = jnp.pad(coords, ((RANGE, RANGE), (0, 0), (0, 0)))
    skel_points = jnp.take_along_axis(coords, leaf_skeleton[:, :, None], axis=1)
    far_tiles = []
    for level in range(LEVELS):
        node_count = LEAVES >> level
        paired = skel_points.reshape(node_count // 2, 2, SKEL, DIM)
        sibling = paired[:, ::-1].reshape(node_count, SKEL, DIM)
        far_tiles.append(pair_kernel(sibling, skel_points))
        if level + 1 < LEVELS:
            first_row = LEAVES - 2 * (LEAVES >> level + 1)
            picked = node_skeleton[first_row:first_row + node_count // 2]
            skel_points = jnp.take_along_axis(paired.reshape(node_count // 2, 2 * SKEL, DIM), picked[:, :, None], axis=1)

    def gains_of(level):
        first_row = 2 * LEAVES - 2 * (LEAVES >> level)
        return node_gain[first_row:first_row + (LEAVES >> level)]

    def sibling_of(values):
        node_count = values.shape[0]
        return values.reshape(node_count // 2, 2, CLASSES, SKEL)[:, ::-1].reshape(node_count, CLASSES, SKEL)

    def operate(vector):
        by_leaf = vector.reshape(CLASSES, LEAVES, LEAF).transpose(1, 0, 2)
        padded_rows = jnp.pad(by_leaf, ((RANGE, RANGE), (0, 0), (0, 0)))

        def near_leaf(leaf_id):
            own_coords = lax.dynamic_index_in_dim(padded_coords, leaf_id + RANGE, 0, keepdims=False)
            total = jnp.zeros((CLASSES, LEAF), jnp.float32)
            for slot_id in range(2 * RANGE + 1):
                other_coords = lax.dynamic_index_in_dim(padded_coords, leaf_id + slot_id, 0, keepdims=False)
                other_rows = lax.dynamic_index_in_dim(padded_rows, leaf_id + slot_id, 0, keepdims=False)
                tile = pair_kernel(other_coords[None], own_coords[None])[0]
                total = total + near_mask[leaf_id, slot_id] * jnp.dot(other_rows, tile, precision=highest)
            return total
        near = lax.map(near_leaf, jnp.arange(LEAVES, dtype=jnp.int32))
        weights = jnp.einsum('ncq,nqs->ncs', by_leaf, leaf_interp, precision=highest)
        weight_levels = [weights]
        for level in range(LEVELS - 1):
            node_count = LEAVES >> level
            scaled = weights.reshape(node_count // 2, 2, CLASSES, SKEL) * gains_of(level).reshape(node_count // 2, 2, 1, SKEL)
            weights = jnp.einsum('ncs,st->nct', scaled[:, 0], transfer[level, 0], precision=highest)
            weights = weights + jnp.einsum('ncs,st->nct', scaled[:, 1], transfer[level, 1], precision=highest)
            weight_levels.append(weights)
        top = LEVELS - 1
        potential = jnp.einsum('ncs,nst->nct', sibling_of(weight_levels[top]), far_tiles[top], precision=highest)
        for level in range(LEVELS - 2, -1, -1):
            node_count = LEAVES >> level
            children = jnp.stack([jnp.einsum('nct,st->ncs', potential, transfer[level, 0], precision=highest), jnp.einsum('nct,st->ncs', potential, transfer[level, 1], precision=highest)], axis=1)
            children = children.reshape(node_count, CLASSES, SKEL) * gains_of(level)[:, None, :]
            potential = children + jnp.einsum('ncs,nst->nct', sibling_of(weight_levels[level]), far_tiles[level], precision=highest)
        far = jnp.einsum('ncs,nqs->ncq', potential, leaf_interp, precision=highest)
        near_flat = near.transpose(1, 0, 2).reshape(CLASSES, POINTS)
        far_flat = far.transpose(1, 0, 2).reshape(CLASSES, POINTS)
        return ridge * vector + near_flat + far_flat
    solution = jnp.zeros_like(right_side)
    residual = right_side
    direction = right_side
    res_norm = symmetric(jnp.dot(residual, residual.T, precision=highest))
    for step in range(ITERS):
        image = operate(direction)
        curvature = symmetric(jnp.dot(direction, image.T, precision=highest))
        alpha_mat = chol_apply(curvature, res_norm)
        solution = solution + jnp.dot(alpha_mat.T, direction, precision=highest)
        residual = residual - jnp.dot(alpha_mat.T, image, precision=highest)
        if step + 1 < ITERS:
            new_norm = symmetric(jnp.dot(residual, residual.T, precision=highest))
            beta_mat = chol_apply(res_norm, new_norm)
            direction = residual + jnp.dot(beta_mat.T, direction, precision=highest)
            res_norm = new_norm
    return (solution, residual)
```

```python
import functools

import jax
import jax.numpy as jnp
from jax import lax
from jax.experimental import pallas as pl
from jax.experimental.pallas import tpu as pltpu
from jax.sharding import PartitionSpec as P

MESH = pl.DeviceIdType.MESH
F32 = jnp.float32
BF16 = jnp.bfloat16
I32 = jnp.int32

LEAF, SKEL, DIM, CLS = 512, 256, 128, 64
LV = 8
LEAVES = 1024
HALF = CLS // 2
OWN = 2 * LEAF
WIDE = (LV + 4) * LEAF


def split(x):
    high = x.astype(BF16)
    return high, (x - high.astype(F32)).astype(BF16)


def dot(a, b, ca=1, cb=0):
    return lax.dot_general(a, b, (((ca,), (cb,)), ((), ())), preferred_element_type=F32)


def times(stacked, high, low, cb=0):
    rows = stacked.shape[0] // 2
    both = dot(stacked, high, 1, cb)
    return both[:rows] + both[rows:] + dot(stacked[:rows], low, 1, cb)


def stack(x):
    return jnp.concatenate(split(x), axis=0)


def times_f32(a, b, cb=0):
    high, low = split(b)
    return times(stack(a), high, low, cb)


def norm_columns(x):
    half = -0.5 * jnp.sum(x * x, axis=1, keepdims=True)
    half = jnp.broadcast_to(half, x.shape)
    first = half.astype(BF16).astype(F32)
    rest = half - first
    second = rest.astype(BF16).astype(F32)
    third = rest - second
    lane = lax.broadcasted_iota(I32, x.shape, 1)
    parts = jnp.where(lane % 3 == 0, first, jnp.where(lane % 3 == 1, second, third))
    ones = jnp.ones_like(parts)
    zero = jnp.zeros_like(parts)
    low = jnp.where(lane < 3, ones, jnp.where(lane < 6, parts, zero))
    high = jnp.where(lane < 3, parts, jnp.where(lane < 6, ones, zero))
    return low.astype(BF16), high.astype(BF16)


def exponent(a_hl, a_n1, b_hl, b_n2):
    a_h = a_hl[:, :DIM]
    b_h, b_l = b_hl[:, :DIM], b_hl[:, DIM:]
    first = dot(a_hl, jnp.concatenate([b_h, b_h], axis=1), 1, 1)
    second = dot(
        jnp.concatenate([a_h, a_n1], axis=1), jnp.concatenate([b_l, b_n2], axis=1), 1, 1
    )
    return first + second


def transposed(top):
    return jnp.concatenate([top, jnp.zeros_like(top)], axis=0).T


def solve(matrix, target):
    work = jnp.concatenate([matrix, target], axis=1)
    row_id = lax.broadcasted_iota(I32, work.shape, 0)
    block = 4
    for start in range(0, CLS, block):
        columns = [
            jnp.broadcast_to(work[:, start + i : start + i + 1], work.shape) for i in range(block)
        ]
        for i in range(block):
            k = start + i
            here = row_id == k
            inverse = 1.0 / columns[i][k : k + 1, :]
            pivot = work[k : k + 1, :] * inverse
            work = jnp.where(here, pivot, work - columns[i] * pivot)
            for j in range(i + 1, block):
                entry = columns[j][k : k + 1, :] * inverse
                columns[j] = jnp.where(here, entry, columns[j] - columns[i] * entry)
    return work


def body(
    points, right_side, neighbours, leaf_interp, leaf_skeleton, node_skeleton, node_gain, transfer,
    x_out, r_out,
    xe, xhl, n1, n2, tile_h, tile_l, be, ye, near, dirn, vs, itp, tra, gw, nw, lsk, idx_rows, idx_cols,
    fh, fl, s_r0, s_q, w_r0, w_q, u4, ar_r0, ar_q,
    local_sem, send_sem, recv_sem,
):
    me = lax.axis_index("leaf")
    core = me % 2
    chip = me // 2
    left = (me + 127) % 128
    right = (me + 1) % 128
    partner = me + 1 - 2 * core

    def peer(axis, s):
        stride = (2, 8, 32)[axis]
        at = (me // stride) % 4
        if s == 1:
            other = at + 1 - 2 * (at % 2)
        elif s == 2:
            other = at + 2 - 4 * (at // 2)
        else:
            other = 3 - at
        return me + (other - at) * stride

    def xor(n, s):
        if s == 1:
            return n + 1 - 2 * (n % 2)
        if s == 2:
            return n + 2 - 4 * ((n // 2) % 2)
        return xor(xor(n, 1), 2)

    loads = []

    def load(src, dst):
        copy = pltpu.make_async_copy(src, dst, local_sem.at[len(loads)])
        copy.start()
        loads.append(copy)
        return copy

    own_rows = pl.ds(OWN, LV * LEAF)
    load_points = load(points, xe.at[own_rows, :])
    load_b = load(right_side, be.at[:, own_rows])
    load_small = [load(leaf_skeleton, lsk)]

    def gain_row(level):
        return 2 * LEAVES - 2 * (LEAVES >> level)

    def skel_row(level):
        return LEAVES - 2 * (LEAVES >> level)

    gain_node = [me * 8, me * 4, me * 2, me, me // 2, me // 4, me // 8, me // 16, me // 32]
    for level in range(9):
        if level < 8:
            at = pl.multiple_of(gain_row(level) + (gain_node[level] // 8) * 8, 8)
            load_small.append(load(node_gain.at[pl.ds(at, 8), :], gw.at[level]))
        else:
            load_small.append(load(node_gain.at[pl.ds(2040, 6), :], gw.at[level, pl.ds(0, 6), :]))
    skel_node = [None, me * 4, me * 2, me, me // 2, me // 4, me // 8, me // 16]
    for level in range(1, 9):
        if level < 8:
            at = pl.multiple_of(skel_row(level) + (skel_node[level] // 8) * 8, 8)
            load_small.append(load(node_skeleton.at[pl.ds(at, 8), :], nw.at[level]))
        else:
            load_small.append(load(node_skeleton.at[pl.ds(1016, 6), :], nw.at[level, pl.ds(0, 6), :]))
    load_itp = load(leaf_interp, itp)
    load_tra = load(transfer, tra)

    peers = [partner, left, right] + [peer(a, s) for a in range(3) for s in (1, 2, 3)]
    barrier = pltpu.get_barrier_semaphore()
    for other in peers:
        pl.semaphore_signal(barrier, inc=1, device_id=(other,), device_id_type=MESH)
    pl.semaphore_wait(barrier, len(peers))

    sent = []

    def send(src, dst, device):
        k = len(sent)
        copy = pltpu.make_async_remote_copy(
            src_ref=src, dst_ref=dst, send_sem=send_sem.at[k], recv_sem=recv_sem.at[k],
            device_id=(device,), device_id_type=MESH,
        )
        copy.start()
        sent.append(copy)
        return copy

    def send_quad(buf, index, axis):
        return [send(buf.at[index, 0], buf.at[index, s], peer(axis, s)) for s in (1, 2, 3)]

    def arrive(copies):
        for copy in copies:
            copy.wait_recv()

    load_points.wait()
    first, last = pl.ds(OWN, OWN), pl.ds(OWN + (LV - 2) * LEAF, OWN)
    head, tail = pl.ds(0, OWN), pl.ds(OWN + LV * LEAF, OWN)
    halo_x = [send(xe.at[first, :], xe.at[tail, :], left), send(xe.at[last, :], xe.at[head, :], right)]
    load_b.wait()
    halo_b = [send(be.at[:, first], be.at[:, tail], left), send(be.at[:, last], be.at[:, head], right)]

    def prepare(e):
        rows = pl.ds(pl.multiple_of(e * LEAF, LEAF), LEAF)
        x = xe[rows, :]
        high, low = split(x)
        xhl[rows, :] = jnp.concatenate([high, low], axis=1)
        a, b = norm_columns(x)
        n1[rows, :] = a
        n2[rows, :] = b

    def split_columns(src, e):
        cols = pl.ds(pl.multiple_of(e * LEAF, LEAF), LEAF)
        high, low = split(src[:, cols])
        vs[pl.ds(0, CLS), cols] = high
        vs[pl.ds(CLS, CLS), cols] = low

    def loop(start, stop, f):
        def step(i, carry):
            f(i)
            return carry

        lax.fori_loop(start, stop, step, 0)

    def own_setup(e):
        prepare(e)
        split_columns(be, e)

    loop(2, 10, own_setup)

    for copy in load_small:
        copy.wait()
    idx_rows[...] = jnp.zeros_like(idx_rows)
    idx_rows[pl.ds(0, 8), :] = lsk[...].astype(F32)

    def put_index(slot, level, row, parity):
        index = nw[level, pl.ds(row, 1), :] + 256 * parity
        index = jnp.where(index >= 512, index - 512, index)
        idx_rows[pl.ds(slot, 1), :] = index.astype(F32)

    for i in range(4):
        put_index(8 + i, 1, (me * 4) % 8 + i, 0)
    for i in range(2):
        put_index(12 + i, 2, (me * 2) % 8 + i, 0)
    put_index(14, 3, me % 8, 0)
    put_index(15, 4, (me // 2) % 8, me % 2)
    n4, n6, n8 = me // 2, me // 8, me // 32
    quad_level = (4, 6, 8)
    quad_node = (n4, n6, n8)
    for q in range(3):
        level, node = quad_level[q], quad_node[q]
        parent = node // 2
        lv = min(level + 1, 8)
        base = 4 if level == 8 else 0
        put_index(16 + 3 * q, lv, base + parent % 8, node % 2)
        put_index(17 + 3 * q, lv, base + xor(parent, 1) % 8, node % 2)
        if q < 2:
            grand = parent // 2
            put_index(18 + 3 * q, level + 2, grand % 8, parent % 2)
    idx_cols[...] = idx_rows[...].T.astype(I32)

    def pick(slot, rows_hl):
        lane = lax.broadcasted_iota(I32, (SKEL, 2 * SKEL), 1)
        chosen = jnp.broadcast_to(idx_cols[:, slot : slot + 1], (SKEL, 2 * SKEL))
        one_hot = jnp.where(lane == chosen, 1.0, 0.0).astype(BF16)
        return dot(one_hot, rows_hl).astype(BF16)

    def joined(hl):
        return hl[:, :DIM].astype(F32) + hl[:, DIM:].astype(F32)

    def far_tile(slot, sibling_hl, own_hl):
        a1, _ = norm_columns(joined(sibling_hl))
        _, b2 = norm_columns(joined(own_hl))
        high, low = split(jnp.exp(exponent(sibling_hl, a1, own_hl, b2)))
        fh[slot] = high
        fl[slot] = low

    skel = [pick(j, xhl[pl.ds(OWN + j * LEAF, LEAF), :]) for j in range(LV)]
    slot, index = 0, 8
    while len(skel) > 1:
        parents = []
        for i in range(len(skel) // 2):
            far_tile(slot, skel[2 * i + 1], skel[2 * i])
            parents.append(pick(index, jnp.concatenate(skel[2 * i : 2 * i + 2], axis=0)))
            slot += 1
            index += 1
        skel = parents
    skel3 = skel[0]
    s_r0[0] = joined(skel3)
    copy_s = [send(s_r0.at[0], s_r0.at[1], partner)]

    def gain(level, node):
        row = node % 8
        return gw[level, pl.ds(row, 1), :]

    load_itp.wait()
    load_tra.wait()

    class Tree:
        pass

    def up_local(it):
        t = Tree()
        t.levels = []
        rows = []
        for j in range(LV):
            v = vs[:, pl.ds(OWN + j * LEAF, LEAF)]
            high, low = split(itp[j])
            rows.append(times(v, high, low))
        for level in range(3):
            t.levels.append(rows)
            count = len(rows)
            lefts = jnp.concatenate(
                [rows[n] * gain(level, me * count + n) for n in range(0, count, 2)], axis=0
            )
            rights = jnp.concatenate(
                [rows[n] * gain(level, me * count + n) for n in range(1, count, 2)], axis=0
            )
            joint = times_f32(lefts, tra[level, 0]) + times_f32(rights, tra[level, 1])
            rows = [joint[n * CLS : (n + 1) * CLS] for n in range(count // 2)]
        w_r0[it, 0] = rows[0]
        t.copies = [send(w_r0.at[it, 0], w_r0.at[it, 1], partner)]
        return t

    my_half = pl.ds(pl.multiple_of(core * HALF, HALF), HALF)

    def up_core(it, t):
        arrive(t.copies)
        own = w_r0[it, 0, my_half, :] * gain(3, me)
        sib = w_r0[it, 1, my_half, :] * gain(3, partner)
        w_q[it * 3, 0] = times_f32(own, tra[3, core]) + times_f32(sib, tra[3, 1 - core])
        t.copies = send_quad(w_q, it * 3, 0)
        t.sib = {}

    def up_quad(it, t, q):
        arrive(t.copies)
        level, node = quad_level[q], quad_node[q]
        parity = node % 2
        four = [w_q[it * 3 + q, s] for s in range(4)]
        t.sib[level] = four[1]
        if q == 2:
            a = four[2] * gain(level, xor(node, 2))
            b = four[3] * gain(level, xor(node, 3))
            t.sib[level + 1] = times_f32(a, tra[level, parity]) + times_f32(b, tra[level, 1 - parity])
            return
        a = jnp.concatenate([four[0] * gain(level, node), four[2] * gain(level, xor(node, 2))], axis=0)
        b = jnp.concatenate(
            [four[1] * gain(level, xor(node, 1)), four[3] * gain(level, xor(node, 3))], axis=0
        )
        two = times_f32(a, tra[level, parity]) + times_f32(b, tra[level, 1 - parity])
        t.sib[level + 1] = two[HALF:]
        parent = node // 2
        parity = parent % 2
        a = two[:HALF] * gain(level + 1, parent)
        b = two[HALF:] * gain(level + 1, xor(parent, 1))
        w_q[it * 3 + q + 1, 0] = times_f32(a, tra[level + 1, parity]) + times_f32(
            b, tra[level + 1, 1 - parity]
        )
        t.copies = send_quad(w_q, it * 3 + q + 1, q + 1)

    def down_top(it, t):
        pot = times(stack(t.sib[9]), fh[13], fl[13])
        for level in range(8, 3, -1):
            node = me // (1 << (level - 3))
            pot = times_f32(pot, tra[level, node % 2], 1) * gain(level, node)
            pot = pot + times(stack(t.sib[level]), fh[level + 4], fl[level + 4])
        u4[it, my_half, :] = pot
        t.copies = [send(u4.at[it, my_half, :], u4.at[it, my_half, :], partner)]

    def down_local(it, t, store):
        arrive(t.copies)
        pot = times_f32(u4[it], tra[3, core], 1) * gain(3, me)
        pot = pot + times(stack(w_r0[it, 1]), fh[7], fl[7])
        slot = 7
        for level in (2, 1, 0):
            rows = t.levels[level]
            count = len(rows)
            slot -= count // 2
            stacked = stack(pot)
            out = []
            lefts = times(stacked, *split(tra[level, 0]), 1)
            rights = times(stacked, *split(tra[level, 1]), 1)
            for n in range(count):
                part = (lefts, rights)[n % 2][(n // 2) * CLS : (n // 2 + 1) * CLS]
                part = part * gain(level, me * count + n)
                other = stack(rows[n + 1 - 2 * (n % 2)])
                f = slot + n // 2
                out.append(part + times(other, fh[f], fl[f], n % 2))
            pot = jnp.concatenate(out, axis=0)
        for j in range(LV):
            high, low = split(itp[j])
            store(j, times(stack(pot[j * CLS : (j + 1) * CLS]), high, low, 1))

    def skel_core():
        arrive(copy_s)
        other = jnp.concatenate(split(s_r0[1]), axis=1)
        far_tile(7, other, skel3)
        own = pick(15, jnp.concatenate([skel3, other], axis=0))
        s_q[0, 0] = joined(own)
        return own, send_quad(s_q, 0, 0)

    def skel_quad(q, own, copies):
        arrive(copies)
        s1, s2, s3 = [jnp.concatenate(split(s_q[q, s]), axis=1) for s in (1, 2, 3)]
        far_tile(8 + 2 * q, s1, own)
        mine = pick(16 + 3 * q, jnp.concatenate([own, s1], axis=0))
        theirs = pick(17 + 3 * q, jnp.concatenate([s2, s3], axis=0))
        far_tile(9 + 2 * q, theirs, mine)
        if q == 2:
            return None, None
        up = pick(18 + 3 * q, jnp.concatenate([mine, theirs], axis=0))
        s_q[q + 1, 0] = joined(up)
        return up, send_quad(s_q, q + 1, q + 1)

    def build(t):
        e = (t + 6) // 3
        k = (t + 6) % 3
        rows = pl.ds(pl.multiple_of(e * LEAF, LEAF), LEAF)
        cols = pl.ds(pl.multiple_of((e + k) * LEAF, LEAF), LEAF)
        if isinstance(t, int):
            flag = neighbours[e - 2, 2 + k] if e >= 2 else neighbours[e + k - 2, 2 - k]
        else:
            flag = neighbours[e - 2, 2 + k]
        mask = jnp.where(flag >= 0, 1.0, 0.0).astype(F32)
        high, low = split(jnp.exp(exponent(xhl[rows, :], n1[rows, :], xhl[cols, :], n2[cols, :])) * mask)
        tile_h[t + 4] = high
        tile_l[t + 4] = low

    def near_target(out, j):
        total = None
        for o in (0, -1, -2, 1, 2):
            cols = pl.ds(pl.multiple_of((j + 2 + o) * LEAF, LEAF), LEAF)
            t = 3 * j + o if o >= 0 else 3 * (j + o) - o
            part = times(vs[:, cols], tile_h[t + 4], tile_l[t + 4], 1 if o > 0 else 0)
            total = part if total is None else total + part
        return total

    def gram(pairs):
        sums = None
        for j in range(LV):
            stacks = {}

            def get(ref, at):
                if id(ref) not in stacks:
                    stacks[id(ref)] = stack(ref[:, pl.ds(at + j * LEAF, LEAF)])
                return stacks[id(ref)]

            parts = []
            for a, a0, b, b0 in pairs:
                bs = get(b, b0)
                parts.append(times(get(a, a0), bs[:CLS], bs[CLS:], 1))
            sums = parts if sums is None else [s + p for s, p in zip(sums, parts)]
        return sums

    class Sum:
        pass

    def sum_start(index, value):
        r = Sum()
        rows = value.shape[0]
        r.rows, r.index = pl.ds(0, rows), index
        ar_r0[index, 0, r.rows, :] = value
        r.copies = [send(ar_r0.at[index, 0, r.rows, :], ar_r0.at[index, 1, r.rows, :], partner)]
        return r

    def sum_step(r, stage):
        arrive(r.copies)
        if stage == 0:
            value = ar_r0[r.index, 0, r.rows, :] + ar_r0[r.index, 1, r.rows, :]
        else:
            at = r.index * 3 + stage - 1
            value = (ar_q[at, 0, r.rows, :] + ar_q[at, 1, r.rows, :]) + (
                ar_q[at, 2, r.rows, :] + ar_q[at, 3, r.rows, :]
            )
        if stage < 3:
            at = r.index * 3 + stage
            ar_q[at, 0, r.rows, :] = value
            r.copies = [
                send(ar_q.at[at, 0, r.rows, :], ar_q.at[at, s, r.rows, :], peer(stage, s)) for s in (1, 2, 3)
            ]
        return value

    def folded(m):
        return jnp.concatenate([m[:HALF], m[HALF:]], axis=1)

    def unfolded(m):
        return jnp.concatenate([m[:, :CLS], m[:, CLS:]], axis=0)

    t0 = up_local(0)
    sum0 = sum_start(0, folded(gram([(be, OWN, be, OWN)])[0]))
    loop(0, 5, build)
    up_core(0, t0)
    own4, copy_s = skel_core()
    sum_step(sum0, 0)
    loop(5, 10, build)
    up_quad(0, t0, 0)
    own6, copy_s = skel_quad(0, own4, copy_s)
    sum_step(sum0, 1)
    loop(10, 15, build)
    up_quad(0, t0, 1)
    own8, copy_s = skel_quad(1, own6, copy_s)
    sum_step(sum0, 2)
    loop(15, 20, build)
    up_quad(0, t0, 2)
    skel_quad(2, own8, copy_s)
    m0 = unfolded(sum_step(sum0, 3))
    down_top(0, t0)
    arrive(halo_x)

    def halo_setup(e):
        prepare(e)

    loop(0, 2, halo_setup)
    loop(10, 12, halo_setup)
    loop(20, 24, build)
    for t in (-4, -2, -1):
        build(t)

    def store_first(j, far):
        cols = pl.ds(OWN + j * LEAF, LEAF)
        ye[:, cols] = far + be[:, cols]

    down_local(0, t0, store_first)
    arrive(halo_b)

    def split_b(e):
        split_columns(be, e)

    loop(0, 2, split_b)
    loop(10, 12, split_b)

    def first_near(j):
        cols = pl.ds(pl.multiple_of((j + 2) * LEAF, LEAF), LEAF)
        ye[:, cols] = ye[:, cols] + near_target(ye, j)

    loop(0, LV, first_near)

    halo_y = [send(ye.at[:, first], ye.at[:, tail], left), send(ye.at[:, last], ye.at[:, head], right)]

    def split_y(e):
        split_columns(ye, e)

    loop(2, 10, split_y)
    t1 = up_local(1)
    sum1 = sum_start(1, jnp.concatenate(gram([(be, OWN, ye, OWN), (ye, OWN, ye, OWN)]), axis=1))

    def second_near(j):
        cols = pl.ds(pl.multiple_of(j * LEAF, LEAF), LEAF)
        near[:, cols] = near_target(near, j)

    loop(2, 4, second_near)
    up_core(1, t1)
    sum_step(sum1, 0)
    loop(4, 5, second_near)
    up_quad(1, t1, 0)
    sum_step(sum1, 1)
    loop(5, 6, second_near)
    up_quad(1, t1, 1)
    sum_step(sum1, 2)
    arrive(halo_y)
    loop(0, 2, split_y)
    loop(10, 12, split_y)
    loop(0, 2, second_near)
    up_quad(1, t1, 2)
    down_top(1, t1)
    moments = sum_step(sum1, 3)
    loop(6, 8, second_near)

    def store_second(j, far):
        cols = pl.ds(j * LEAF, LEAF)
        near[:, cols] = near[:, cols] + far + ye[:, pl.ds(OWN + j * LEAF, LEAF)]

    down_local(1, t1, store_second)

    def square_t(m):
        return jnp.concatenate([m, jnp.zeros_like(m)], axis=1)

    def sym(m):
        return 0.5 * (m + transposed(square_t(m))[:CLS, :CLS])

    m0 = sym(m0)
    m1 = moments[:, :CLS]
    m2 = moments[:, CLS:]
    step = solve(sym(m1), m0)
    alpha = step[:, CLS:]
    alpha_t = transposed(step)[CLS:, :CLS]
    cross = times_f32(m1, alpha)
    new = m0 - 2.0 * sym(cross) + sym(times_f32(times_f32(alpha_t, m2), alpha))
    beta_t = transposed(solve(m0, new))[CLS:, :CLS]
    row = lax.broadcasted_iota(I32, (CLS, CLS), 0)
    col = lax.broadcasted_iota(I32, (CLS, CLS), 1)
    plus_t = jnp.where(row == col, 1.0, 0.0) + beta_t

    alpha_s = stack(alpha_t)
    plus_s = stack(plus_t)

    def mix(matrix_s, x):
        high, low = split(x)
        return times(matrix_s, high, low)

    def make_second(j):
        cols = pl.ds(pl.multiple_of(j * LEAF, LEAF), LEAF)
        wide = pl.ds(pl.multiple_of((j + 2) * LEAF, LEAF), LEAF)
        dirn[:, cols] = mix(plus_s, be[:, wide]) - mix(alpha_s, ye[:, wide])
        near[:, cols] = mix(plus_s, ye[:, wide]) - mix(alpha_s, near[:, cols])

    loop(0, LV, make_second)
    curve = sum_start(2, folded(gram([(dirn, 0, near, 0)])[0]))

    def first_update(j):
        wide = pl.ds(pl.multiple_of((j + 2) * LEAF, LEAF), LEAF)
        old = be[:, wide]
        be[:, wide] = mix(alpha_s, old)
        ye[:, wide] = old - mix(alpha_s, ye[:, wide])

    sum_step(curve, 0)
    for copy in halo_b + halo_y:
        copy.wait_send()
    loop(0, LV, first_update)
    sum_step(curve, 1)
    sum_step(curve, 2)
    curvature = sym(unfolded(sum_step(curve, 3)))
    last_t = transposed(solve(curvature, new))[CLS:, :CLS]
    last_s = stack(last_t)

    def last_update(j):
        cols = pl.ds(pl.multiple_of(j * LEAF, LEAF), LEAF)
        wide = pl.ds(pl.multiple_of((j + 2) * LEAF, LEAF), LEAF)
        be[:, wide] = be[:, wide] + mix(last_s, dirn[:, cols])
        ye[:, wide] = ye[:, wide] - mix(last_s, near[:, cols])

    loop(0, LV, last_update)
    outs = [load(be.at[:, own_rows], x_out), load(ye.at[:, own_rows], r_out)]
    for copy in outs:
        copy.wait()
    for copy in sent:
        if not any(copy is done for done in halo_b + halo_y):
            copy.wait_send()


def solution(mesh):
    any_space = pl.BlockSpec(memory_space=pl.ANY)
    vmem = pltpu.VMEM

    def device(points, right_side, neighbours, leaf_interp, leaf_skeleton, node_skeleton, node_gain, transfer):
        out = jax.ShapeDtypeStruct(right_side.shape, F32)
        return pl.pallas_call(
            body,
            out_shape=(out, out),
            in_specs=[
                any_space, any_space, pl.BlockSpec(memory_space=pltpu.SMEM), any_space,
                any_space, any_space, any_space, any_space,
            ],
            out_specs=(any_space, any_space),
            scratch_shapes=[
                vmem((WIDE, DIM), F32),
                vmem((WIDE, 2 * DIM), BF16),
                vmem((WIDE, DIM), BF16),
                vmem((WIDE, DIM), BF16),
                vmem((28, LEAF, LEAF), BF16),
                vmem((28, LEAF, LEAF), BF16),
                vmem((CLS, WIDE), F32),
                vmem((CLS, WIDE), F32),
                vmem((CLS, LV * LEAF), F32),
                vmem((CLS, LV * LEAF), F32),
                vmem((2 * CLS, WIDE), BF16),
                vmem((LV, LEAF, SKEL), F32),
                vmem((9, 2, SKEL, SKEL), F32),
                vmem((9, 8, SKEL), F32),
                vmem((9, 8, SKEL), I32),
                vmem((LV, SKEL), I32),
                vmem((128, SKEL), F32),
                vmem((SKEL, 128), I32),
                vmem((14, SKEL, SKEL), BF16),
                vmem((14, SKEL, SKEL), BF16),
                vmem((2, SKEL, DIM), F32),
                vmem((3, 4, SKEL, DIM), F32),
                vmem((2, 2, CLS, SKEL), F32),
                vmem((6, 4, HALF, SKEL), F32),
                vmem((2, CLS, SKEL), F32),
                vmem((3, 2, CLS, 128), F32),
                vmem((9, 4, CLS, 128), F32),
                pltpu.SemaphoreType.DMA((26,)),
                pltpu.SemaphoreType.DMA((70,)),
                pltpu.SemaphoreType.DMA((70,)),
            ],
            compiler_params=pltpu.CompilerParams(
                collective_id=0, has_side_effects=True, vmem_limit_bytes=67043328
            ),
        )(points, right_side, neighbours, leaf_interp, leaf_skeleton, node_skeleton, node_gain, transfer)

    in_specs = (
        P("leaf", None), P(None, "leaf"), P("leaf", None), P("leaf", None, None),
        P("leaf", None), P(), P(), P(),
    )
    out_specs = (P(None, "leaf"), P(None, "leaf"))
    return jax.shard_map(device, mesh=mesh, in_specs=in_specs, out_specs=out_specs, check_vma=False)
```

```python
import functools

import jax
import jax.numpy as jnp
from jax import lax
from jax.experimental import pallas as pl
from jax.experimental.pallas import tpu as pltpu
from jax.sharding import PartitionSpec as P

MESH = pl.DeviceIdType.MESH
F32 = jnp.float32
BF16 = jnp.bfloat16
I32 = jnp.int32

LEAF, SKEL, DIM, CLS = 512, 256, 128, 64
LV = 8
LEAVES = 1024
HALF = CLS // 2
OWN = 2 * LEAF
WIDE = (LV + 4) * LEAF


def split(x):
    high = x.astype(BF16)
    return high, (x - high.astype(F32)).astype(BF16)


def dot(a, b, ca=1, cb=0):
    return lax.dot_general(a, b, (((ca,), (cb,)), ((), ())), preferred_element_type=F32)


def times(stacked, high, low, cb=0):
    rows = stacked.shape[0] // 2
    both = dot(stacked, high, 1, cb)
    return both[:rows] + both[rows:] + dot(stacked[:rows], low, 1, cb)


def stack(x):
    return jnp.concatenate(split(x), axis=0)


def times_f32(a, b, cb=0):
    high, low = split(b)
    return times(stack(a), high, low, cb)


def norm_columns(x):
    half = -0.5 * jnp.sum(x * x, axis=1, keepdims=True)
    half = jnp.broadcast_to(half, x.shape)
    first = half.astype(BF16).astype(F32)
    rest = half - first
    second = rest.astype(BF16).astype(F32)
    third = rest - second
    lane = lax.broadcasted_iota(I32, x.shape, 1)
    parts = jnp.where(lane % 3 == 0, first, jnp.where(lane % 3 == 1, second, third))
    ones = jnp.ones_like(parts)
    zero = jnp.zeros_like(parts)
    low = jnp.where(lane < 3, ones, jnp.where(lane < 6, parts, zero))
    high = jnp.where(lane < 3, parts, jnp.where(lane < 6, ones, zero))
    return low.astype(BF16), high.astype(BF16)


def exponent(a_hl, a_n1, b_hl, b_n2):
    a_h = a_hl[:, :DIM]
    b_h, b_l = b_hl[:, :DIM], b_hl[:, DIM:]
    first = dot(a_hl, jnp.concatenate([b_h, b_h], axis=1), 1, 1)
    second = dot(
        jnp.concatenate([a_h, a_n1], axis=1), jnp.concatenate([b_l, b_n2], axis=1), 1, 1
    )
    return first + second


def transposed(top):
    return jnp.concatenate([top, jnp.zeros_like(top)], axis=0).T


def solve(matrix, target):
    work = jnp.concatenate([matrix, target], axis=1)
    row_id = lax.broadcasted_iota(I32, work.shape, 0)
    block = 4
    for start in range(0, CLS, block):
        columns = [
            jnp.broadcast_to(work[:, start + i : start + i + 1], work.shape) for i in range(block)
        ]
        for i in range(block):
            k = start + i
            here = row_id == k
            inverse = 1.0 / columns[i][k : k + 1, :]
            pivot = work[k : k + 1, :] * inverse
            work = jnp.where(here, pivot, work - columns[i] * pivot)
            for j in range(i + 1, block):
                entry = columns[j][k : k + 1, :] * inverse
                columns[j] = jnp.where(here, entry, columns[j] - columns[i] * entry)
    return work


def body(
    points, right_side, neighbours, leaf_interp, leaf_skeleton, node_skeleton, node_gain, transfer,
    x_out, r_out,
    xe, xhl, n1, n2, tile_h, tile_l, be, ye, near, dirn, vs, itp, tra, gw, nw, lsk, idx_rows, idx_cols,
    fh, fl, s_r0, s_q, w_r0, w_q, u4, ar_r0, ar_q,
    local_sem, send_sem, recv_sem,
):
    me = lax.axis_index("leaf")
    core = me % 2
    chip = me // 2
    left = (me + 127) % 128
    right = (me + 1) % 128
    partner = me + 1 - 2 * core

    def peer(axis, s):
        stride = (2, 8, 32)[axis]
        at = (me // stride) % 4
        if s == 1:
            other = at + 1 - 2 * (at % 2)
        elif s == 2:
            other = at + 2 - 4 * (at // 2)
        else:
            other = 3 - at
        return me + (other - at) * stride

    def xor(n, s):
        if s == 1:
            return n + 1 - 2 * (n % 2)
        if s == 2:
            return n + 2 - 4 * ((n // 2) % 2)
        return xor(xor(n, 1), 2)

    loads = []

    def load(src, dst):
        copy = pltpu.make_async_copy(src, dst, local_sem.at[len(loads)])
        copy.start()
        loads.append(copy)
        return copy

    own_rows = pl.ds(OWN, LV * LEAF)
    load_points = load(points, xe.at[own_rows, :])
    load_small = [load(leaf_skeleton, lsk)]

    def gain_row(level):
        return 2 * LEAVES - 2 * (LEAVES >> level)

    def skel_row(level):
        return LEAVES - 2 * (LEAVES >> level)

    gain_node = [me * 8, me * 4, me * 2, me, me // 2, me // 4, me // 8, me // 16, me // 32]
    for level in range(9):
        if level < 8:
            at = pl.multiple_of(gain_row(level) + (gain_node[level] // 8) * 8, 8)
            load_small.append(load(node_gain.at[pl.ds(at, 8), :], gw.at[level]))
        else:
            load_small.append(load(node_gain.at[pl.ds(2040, 6), :], gw.at[level, pl.ds(0, 6), :]))
    skel_node = [None, me * 4, me * 2, me, me // 2, me // 4, me // 8, me // 16]
    for level in range(1, 9):
        if level < 8:
            at = pl.multiple_of(skel_row(level) + (skel_node[level] // 8) * 8, 8)
            load_small.append(load(node_skeleton.at[pl.ds(at, 8), :], nw.at[level]))
        else:
            load_small.append(load(node_skeleton.at[pl.ds(1016, 6), :], nw.at[level, pl.ds(0, 6), :]))
    load_b = load(right_side, be.at[:, own_rows])
    load_itp = load(leaf_interp, itp)
    load_tra = load(transfer, tra)

    peers = [partner, left, right] + [peer(a, s) for a in range(3) for s in (1, 2, 3)]
    barrier = pltpu.get_barrier_semaphore()
    for other in peers:
        pl.semaphore_signal(barrier, inc=1, device_id=(other,), device_id_type=MESH)

    sent = []

    def send(src, dst, device):
        k = len(sent)
        copy = pltpu.make_async_remote_copy(
            src_ref=src, dst_ref=dst, send_sem=send_sem.at[k], recv_sem=recv_sem.at[k],
            device_id=(device,), device_id_type=MESH,
        )
        copy.start()
        sent.append(copy)
        return copy

    def send_quad(buf, index, axis):
        return [send(buf.at[index, 0], buf.at[index, s], peer(axis, s)) for s in (1, 2, 3)]

    def arrive(copies):
        for copy in copies:
            copy.wait_recv()

    first, last = pl.ds(OWN, OWN), pl.ds(OWN + (LV - 2) * LEAF, OWN)
    head, tail = pl.ds(0, OWN), pl.ds(OWN + LV * LEAF, OWN)

    def halo_rows(ref):
        return [send(ref.at[first, :], ref.at[tail, :], left), send(ref.at[last, :], ref.at[head, :], right)]

    def halo_columns(ref):
        return [send(ref.at[:, first], ref.at[:, tail], left), send(ref.at[:, last], ref.at[:, head], right)]

    def split_rows(e):
        rows = pl.ds(pl.multiple_of(e * LEAF, LEAF), LEAF)
        xhl[rows, :] = jnp.concatenate(split(xe[rows, :]), axis=1)

    def prepare(e):
        rows = pl.ds(pl.multiple_of(e * LEAF, LEAF), LEAF)
        a, b = norm_columns(xe[rows, :])
        n1[rows, :] = a
        n2[rows, :] = b

    def split_columns(src, e):
        cols = pl.ds(pl.multiple_of(e * LEAF, LEAF), LEAF)
        high, low = split(src[:, cols])
        vs[pl.ds(0, CLS), cols] = high
        vs[pl.ds(CLS, CLS), cols] = low

    def loop(start, stop, f):
        def step(i, carry):
            f(i)
            return carry

        lax.fori_loop(start, stop, step, 0)

    load_points.wait()
    loop(2, 10, split_rows)

    for copy in load_small:
        copy.wait()
    idx_rows[...] = jnp.zeros_like(idx_rows)
    idx_rows[pl.ds(0, 8), :] = lsk[...].astype(F32)

    def put_index(slot, level, row, parity):
        index = nw[level, pl.ds(row, 1), :] + 256 * parity
        index = jnp.where(index >= 512, index - 512, index)
        idx_rows[pl.ds(slot, 1), :] = index.astype(F32)

    for i in range(4):
        put_index(8 + i, 1, (me * 4) % 8 + i, 0)
    for i in range(2):
        put_index(12 + i, 2, (me * 2) % 8 + i, 0)
    put_index(14, 3, me % 8, 0)
    put_index(15, 4, (me // 2) % 8, me % 2)
    n4, n6, n8 = me // 2, me // 8, me // 32
    quad_level = (4, 6, 8)
    quad_node = (n4, n6, n8)
    for q in range(3):
        level, node = quad_level[q], quad_node[q]
        parent = node // 2
        lv = min(level + 1, 8)
        base = 4 if level == 8 else 0
        put_index(16 + 3 * q, lv, base + parent % 8, node % 2)
        put_index(17 + 3 * q, lv, base + xor(parent, 1) % 8, node % 2)
        if q < 2:
            grand = parent // 2
            put_index(18 + 3 * q, level + 2, grand % 8, parent % 2)
    idx_cols[...] = idx_rows[...].T.astype(I32)

    def pick(slot, rows_hl):
        lane = lax.broadcasted_iota(I32, (SKEL, 2 * SKEL), 1)
        chosen = jnp.broadcast_to(idx_cols[:, slot : slot + 1], (SKEL, 2 * SKEL))
        one_hot = jnp.where(lane == chosen, 1.0, 0.0).astype(BF16)
        return dot(one_hot, rows_hl).astype(BF16)

    def joined(hl):
        return hl[:, :DIM].astype(F32) + hl[:, DIM:].astype(F32)

    def far_tile(slot, sibling_hl, own_hl):
        a1, _ = norm_columns(joined(sibling_hl))
        _, b2 = norm_columns(joined(own_hl))
        high, low = split(jnp.exp(exponent(sibling_hl, a1, own_hl, b2)))
        fh[slot] = high
        fl[slot] = low

    skel = [pick(j, xhl[pl.ds(OWN + j * LEAF, LEAF), :]) for j in range(LV)]
    index = 8
    pairs = []
    while len(skel) > 1:
        parents = []
        for i in range(len(skel) // 2):
            pairs.append((skel[2 * i + 1], skel[2 * i]))
            parents.append(pick(index, jnp.concatenate(skel[2 * i : 2 * i + 2], axis=0)))
            index += 1
        skel = parents
    skel3 = skel[0]
    s_r0[0] = joined(skel3)
    pl.semaphore_wait(barrier, len(peers))
    copy_s = [send(s_r0.at[0], s_r0.at[1], partner)]

    def gain(level, node):
        row = node % 8
        return gw[level, pl.ds(row, 1), :]

    class Tree:
        pass

    def up_local(it):
        t = Tree()
        t.levels = []
        rows = []
        for j in range(LV):
            v = vs[:, pl.ds(OWN + j * LEAF, LEAF)]
            high, low = split(itp[j])
            rows.append(times(v, high, low))
        for level in range(3):
            t.levels.append(rows)
            count = len(rows)
            lefts = jnp.concatenate(
                [rows[n] * gain(level, me * count + n) for n in range(0, count, 2)], axis=0
            )
            rights = jnp.concatenate(
                [rows[n] * gain(level, me * count + n) for n in range(1, count, 2)], axis=0
            )
            joint = times_f32(lefts, tra[level, 0]) + times_f32(rights, tra[level, 1])
            rows = [joint[n * CLS : (n + 1) * CLS] for n in range(count // 2)]
        w_r0[it, 0] = rows[0]
        t.copies = [send(w_r0.at[it, 0], w_r0.at[it, 1], partner)]
        return t

    my_half = pl.ds(pl.multiple_of(core * HALF, HALF), HALF)

    def up_core(it, t):
        arrive(t.copies)
        own = w_r0[it, 0, my_half, :] * gain(3, me)
        sib = w_r0[it, 1, my_half, :] * gain(3, partner)
        w_q[it * 3, 0] = times_f32(own, tra[3, core]) + times_f32(sib, tra[3, 1 - core])
        t.copies = send_quad(w_q, it * 3, 0)
        t.sib = {}

    def up_quad(it, t, q):
        arrive(t.copies)
        level, node = quad_level[q], quad_node[q]
        parity = node % 2
        four = [w_q[it * 3 + q, s] for s in range(4)]
        t.sib[level] = four[1]
        if q == 2:
            a = four[2] * gain(level, xor(node, 2))
            b = four[3] * gain(level, xor(node, 3))
            t.sib[level + 1] = times_f32(a, tra[level, parity]) + times_f32(b, tra[level, 1 - parity])
            return
        a = jnp.concatenate([four[0] * gain(level, node), four[2] * gain(level, xor(node, 2))], axis=0)
        b = jnp.concatenate(
            [four[1] * gain(level, xor(node, 1)), four[3] * gain(level, xor(node, 3))], axis=0
        )
        two = times_f32(a, tra[level, parity]) + times_f32(b, tra[level, 1 - parity])
        t.sib[level + 1] = two[HALF:]
        parent = node // 2
        parity = parent % 2
        a = two[:HALF] * gain(level + 1, parent)
        b = two[HALF:] * gain(level + 1, xor(parent, 1))
        w_q[it * 3 + q + 1, 0] = times_f32(a, tra[level + 1, parity]) + times_f32(
            b, tra[level + 1, 1 - parity]
        )
        t.copies = send_quad(w_q, it * 3 + q + 1, q + 1)

    def down_top(it, t):
        pot = times(stack(t.sib[9]), fh[13], fl[13])
        for level in range(8, 3, -1):
            node = me // (1 << (level - 3))
            pot = times_f32(pot, tra[level, node % 2], 1) * gain(level, node)
            pot = pot + times(stack(t.sib[level]), fh[level + 4], fl[level + 4])
        u4[it, my_half, :] = pot
        t.copies = [send(u4.at[it, my_half, :], u4.at[it, my_half, :], partner)]

    def down_device(it, t):
        arrive(t.copies)
        pot = times_f32(u4[it], tra[3, core], 1) * gain(3, me)
        t.top = pot + times(stack(w_r0[it, 1]), fh[7], fl[7])

    def tree_gram(t):
        total = None
        slot = 0
        for level in range(3):
            rows = t.levels[level]
            for i in range(len(rows) // 2):
                part = times(stack(rows[2 * i + 1]), fh[slot], fl[slot])
                part = times_f32(rows[2 * i], part, 1)
                total = part if total is None else total + part
                slot += 1
        return total

    def down_local(it, t, store):
        pot = t.top
        slot = 7
        for level in (2, 1, 0):
            rows = t.levels[level]
            count = len(rows)
            slot -= count // 2
            stacked = stack(pot)
            out = []
            lefts = times(stacked, *split(tra[level, 0]), 1)
            rights = times(stacked, *split(tra[level, 1]), 1)
            for n in range(count):
                part = (lefts, rights)[n % 2][(n // 2) * CLS : (n // 2 + 1) * CLS]
                part = part * gain(level, me * count + n)
                other = stack(rows[n + 1 - 2 * (n % 2)])
                f = slot + n // 2
                out.append(part + times(other, fh[f], fl[f], n % 2))
            pot = jnp.concatenate(out, axis=0)
        for j in range(LV):
            high, low = split(itp[j])
            store(j, times(stack(pot[j * CLS : (j + 1) * CLS]), high, low, 1))

    my_points = pl.ds(pl.multiple_of(core * 128, 128), 128)

    def send_skel(q):
        return [
            send(s_q.at[q, 0, my_points, :], s_q.at[q, s, my_points, :], peer(q, s)) for s in (1, 2, 3)
        ]

    def forward_skel(q, copies):
        arrive(copies)
        part = s_q.at[q, pl.ds(1, 3), my_points, :]
        return [send(part, part, partner)]

    def skel_core():
        arrive(copy_s)
        other = jnp.concatenate(split(s_r0[1]), axis=1)
        own = pick(15, jnp.concatenate([skel3, other], axis=0))
        s_q[0, 0] = joined(own)
        return (own, [(7, other, skel3)], send_skel(0))

    def skel_quad(q, own, copies):
        arrive(copies)
        s1, s2, s3 = [jnp.concatenate(split(s_q[q, s]), axis=1) for s in (1, 2, 3)]
        mine = pick(16 + 3 * q, jnp.concatenate([own, s1], axis=0))
        theirs = pick(17 + 3 * q, jnp.concatenate([s2, s3], axis=0))
        tiles = [(8 + 2 * q, s1, own), (9 + 2 * q, theirs, mine)]
        if q == 2:
            return None, tiles, None
        up = pick(18 + 3 * q, jnp.concatenate([mine, theirs], axis=0))
        s_q[q + 1, 0] = joined(up)
        return up, tiles, send_skel(q + 1)

    def far_tiles(tiles):
        for tile in tiles:
            far_tile(*tile)

    def build(t):
        e = (t + 6) // 3
        k = (t + 6) % 3
        rows = pl.ds(pl.multiple_of(e * LEAF, LEAF), LEAF)
        cols = pl.ds(pl.multiple_of((e + k) * LEAF, LEAF), LEAF)
        if isinstance(t, int):
            flag = neighbours[e - 2, 2 + k] if e >= 2 else neighbours[e + k - 2, 2 - k]
        else:
            flag = neighbours[e - 2, 2 + k]
        mask = jnp.where(flag >= 0, 1.0, 0.0).astype(F32)
        high, low = split(jnp.exp(exponent(xhl[rows, :], n1[rows, :], xhl[cols, :], n2[cols, :])) * mask)
        tile_h[t + 4] = high
        tile_l[t + 4] = low

    def near_target(out, j):
        total = None
        for o in (0, -1, -2, 1, 2):
            cols = pl.ds(pl.multiple_of((j + 2 + o) * LEAF, LEAF), LEAF)
            t = 3 * j + o if o >= 0 else 3 * (j + o) - o
            part = times(vs[:, cols], tile_h[t + 4], tile_l[t + 4], 1 if o > 0 else 0)
            total = part if total is None else total + part
        return total

    def gram(pairs):
        sums = None
        for j in range(LV):
            stacks = {}

            def get(ref, at):
                if id(ref) not in stacks:
                    stacks[id(ref)] = stack(ref[:, pl.ds(at + j * LEAF, LEAF)])
                return stacks[id(ref)]

            parts = []
            for a, a0, b, b0 in pairs:
                bs = get(b, b0)
                parts.append(times(get(a, a0), bs[:CLS], bs[CLS:], 1))
            sums = parts if sums is None else [s + p for s, p in zip(sums, parts)]
        return sums

    class Sum:
        pass

    def sum_start(index, value):
        r = Sum()
        rows = value.shape[0]
        r.rows, r.index = pl.ds(0, rows), index
        ar_r0[index, 0, r.rows, :] = value
        r.copies = [send(ar_r0.at[index, 0, r.rows, :], ar_r0.at[index, 1, r.rows, :], partner)]
        return r

    def sum_step(r, stage):
        arrive(r.copies)
        if stage == 0:
            value = ar_r0[r.index, 0, r.rows, :] + ar_r0[r.index, 1, r.rows, :]
        else:
            at = r.index * 3 + stage - 1
            value = (ar_q[at, 0, r.rows, :] + ar_q[at, 1, r.rows, :]) + (
                ar_q[at, 2, r.rows, :] + ar_q[at, 3, r.rows, :]
            )
        if stage < 3:
            at = r.index * 3 + stage
            ar_q[at, 0, r.rows, :] = value
            r.copies = [
                send(ar_q.at[at, 0, r.rows, :], ar_q.at[at, s, r.rows, :], peer(stage, s)) for s in (1, 2, 3)
            ]
        return value

    def folded(m):
        return jnp.concatenate([m[:HALF], m[HALF:]], axis=1)

    def unfolded(m):
        return jnp.concatenate([m[:, :CLS], m[:, CLS:]], axis=0)

    def square_t(m):
        return jnp.concatenate([m, jnp.zeros_like(m)], axis=1)

    def low_pairs_t(m):
        return transposed(square_t(m))[:CLS, :CLS]

    loop(2, 10, prepare)
    far_tiles([(i, *pair) for i, pair in enumerate(pairs)])
    loop(0, 2, build)
    own4, tiles3, copy_s = skel_core()
    load_b.wait()

    def split_b(e):
        split_columns(be, e)

    loop(2, 10, split_b)
    load_itp.wait()
    load_tra.wait()
    t0 = up_local(0)
    sum0 = sum_start(0, folded(gram([(be, OWN, be, OWN)])[0]))
    loop(2, 5, build)
    up_core(0, t0)
    sum_step(sum0, 0)
    far_tiles(tiles3)
    loop(5, 9, build)
    copy_s = forward_skel(0, copy_s)
    halo_x = halo_rows(xe)
    halo_b = halo_columns(be)
    loop(9, 11, build)
    own6, tiles4, copy_s = skel_quad(0, own4, copy_s)
    loop(11, 13, build)
    up_quad(0, t0, 0)
    sum_step(sum0, 1)
    far_tiles(tiles4)
    loop(13, 20, build)
    copy_s = forward_skel(1, copy_s)
    up_quad(0, t0, 1)
    sum_step(sum0, 2)
    own8, tiles6, copy_s = skel_quad(1, own6, copy_s)
    far_tiles(tiles6)
    arrive(halo_x)

    def halo_setup(e):
        split_rows(e)
        prepare(e)

    loop(0, 2, halo_setup)
    loop(10, 12, halo_setup)
    loop(20, 24, build)
    arrive(halo_b)
    copy_s = forward_skel(2, copy_s)
    for t in (-4, -2, -1):
        build(t)
    loop(0, 2, split_b)
    loop(10, 12, split_b)
    up_quad(0, t0, 2)
    m0 = unfolded(sum_step(sum0, 3))
    _, tiles8, _ = skel_quad(2, own8, copy_s)
    far_tiles(tiles8)
    down_top(0, t0)

    def first_near(j):
        cols = pl.ds(pl.multiple_of((j + 2) * LEAF, LEAF), LEAF)
        ye[:, cols] = be[:, cols] + near_target(ye, j)

    loop(0, LV, first_near)
    down_device(0, t0)

    def store_first(j, far):
        cols = pl.ds(OWN + j * LEAF, LEAF)
        ye[:, cols] = ye[:, cols] + far

    down_local(0, t0, store_first)

    def split_y(e):
        split_columns(ye, e)

    loop(2, 10, split_y)
    t1 = up_local(1)
    halo_y = halo_columns(ye)
    sum1 = sum_start(1, jnp.concatenate(gram([(be, OWN, ye, OWN), (ye, OWN, ye, OWN)]), axis=1))

    def second_near(j):
        cols = pl.ds(pl.multiple_of(j * LEAF, LEAF), LEAF)
        near[:, cols] = near_target(near, j)

    up_core(1, t1)
    sum_step(sum1, 0)
    low_pairs = tree_gram(t1)
    loop(2, 6, second_near)
    up_quad(1, t1, 0)
    sum_step(sum1, 1)
    arrive(halo_y)
    loop(0, 2, split_y)
    loop(10, 12, split_y)
    loop(0, 2, second_near)
    loop(6, 8, second_near)
    up_quad(1, t1, 1)
    sum_step(sum1, 2)
    near_gram = gram([(ye, OWN, near, 0)])[0]
    up_quad(1, t1, 2)
    down_top(1, t1)
    moments = sum_step(sum1, 3)
    down_device(1, t1)
    bends = near_gram + low_pairs + low_pairs_t(low_pairs) + times_f32(w_r0[1, 0], t1.top, 1)
    curve = sum_start(2, folded(bends))

    def store_second(j, far):
        cols = pl.ds(j * LEAF, LEAF)
        near[:, cols] = near[:, cols] + far + ye[:, pl.ds(OWN + j * LEAF, LEAF)]

    down_local(1, t1, store_second)

    def sym(m):
        return 0.5 * (m + transposed(square_t(m))[:CLS, :CLS])

    m0 = sym(m0)
    m1 = moments[:, :CLS]
    m2 = moments[:, CLS:]
    step = solve(sym(m1), m0)
    alpha = step[:, CLS:]
    alpha_t = transposed(step)[CLS:, :CLS]
    cross = times_f32(m1, alpha)
    new = m0 - 2.0 * sym(cross) + sym(times_f32(times_f32(alpha_t, m2), alpha))
    beta_t = transposed(solve(m0, new))[CLS:, :CLS]
    row = lax.broadcasted_iota(I32, (CLS, CLS), 0)
    col = lax.broadcasted_iota(I32, (CLS, CLS), 1)
    plus_t = jnp.where(row == col, 1.0, 0.0) + beta_t

    alpha_s = stack(alpha_t)
    plus_s = stack(plus_t)

    def mix(matrix_s, x):
        high, low = split(x)
        return times(matrix_s, high, low)

    def make_second(j):
        cols = pl.ds(pl.multiple_of(j * LEAF, LEAF), LEAF)
        wide = pl.ds(pl.multiple_of((j + 2) * LEAF, LEAF), LEAF)
        dirn[:, cols] = mix(plus_s, be[:, wide]) - mix(alpha_s, ye[:, wide])
        near[:, cols] = mix(plus_s, ye[:, wide]) - mix(alpha_s, near[:, cols])

    sum_step(curve, 0)
    loop(0, LV, make_second)
    sum_step(curve, 1)
    for copy in halo_b + halo_y:
        copy.wait_send()

    def first_update(j):
        wide = pl.ds(pl.multiple_of((j + 2) * LEAF, LEAF), LEAF)
        old = be[:, wide]
        be[:, wide] = mix(alpha_s, old)
        ye[:, wide] = old - mix(alpha_s, ye[:, wide])

    loop(0, LV, first_update)
    plus = transposed(square_t(plus_t))[:CLS, :CLS]
    known = times_f32(times_f32(plus_t, m1), plus) - 2.0 * sym(times_f32(times_f32(plus_t, m2), alpha))
    known = known + times_f32(times_f32(alpha_t, m2), alpha)
    sum_step(curve, 2)
    bends = unfolded(sum_step(curve, 3))
    curvature = sym(known + times_f32(times_f32(alpha_t, bends), alpha))
    last_t = transposed(solve(curvature, new))[CLS:, :CLS]
    last_s = stack(last_t)

    def last_update(j):
        cols = pl.ds(pl.multiple_of(j * LEAF, LEAF), LEAF)
        wide = pl.ds(pl.multiple_of((j + 2) * LEAF, LEAF), LEAF)
        be[:, wide] = be[:, wide] + mix(last_s, dirn[:, cols])
        ye[:, wide] = ye[:, wide] - mix(last_s, near[:, cols])

    loop(0, LV, last_update)
    outs = [load(be.at[:, own_rows], x_out), load(ye.at[:, own_rows], r_out)]
    for copy in outs:
        copy.wait()
    for copy in sent:
        if not any(copy is done for done in halo_b + halo_y):
            copy.wait_send()


def solution(mesh):
    any_space = pl.BlockSpec(memory_space=pl.ANY)
    vmem = pltpu.VMEM

    def device(points, right_side, neighbours, leaf_interp, leaf_skeleton, node_skeleton, node_gain, transfer):
        out = jax.ShapeDtypeStruct(right_side.shape, F32)
        return pl.pallas_call(
            body,
            out_shape=(out, out),
            in_specs=[
                any_space, any_space, pl.BlockSpec(memory_space=pltpu.SMEM), any_space,
                any_space, any_space, any_space, any_space,
            ],
            out_specs=(any_space, any_space),
            scratch_shapes=[
                vmem((WIDE, DIM), F32),
                vmem((WIDE, 2 * DIM), BF16),
                vmem((WIDE, DIM), BF16),
                vmem((WIDE, DIM), BF16),
                vmem((28, LEAF, LEAF), BF16),
                vmem((28, LEAF, LEAF), BF16),
                vmem((CLS, WIDE), F32),
                vmem((CLS, WIDE), F32),
                vmem((CLS, LV * LEAF), F32),
                vmem((CLS, LV * LEAF), F32),
                vmem((2 * CLS, WIDE), BF16),
                vmem((LV, LEAF, SKEL), F32),
                vmem((9, 2, SKEL, SKEL), F32),
                vmem((9, 8, SKEL), F32),
                vmem((9, 8, SKEL), I32),
                vmem((LV, SKEL), I32),
                vmem((128, SKEL), F32),
                vmem((SKEL, 128), I32),
                vmem((14, SKEL, SKEL), BF16),
                vmem((14, SKEL, SKEL), BF16),
                vmem((2, SKEL, DIM), F32),
                vmem((3, 4, SKEL, DIM), F32),
                vmem((2, 2, CLS, SKEL), F32),
                vmem((6, 4, HALF, SKEL), F32),
                vmem((2, CLS, SKEL), F32),
                vmem((3, 2, CLS, 128), F32),
                vmem((9, 4, CLS, 128), F32),
                pltpu.SemaphoreType.DMA((26,)),
                pltpu.SemaphoreType.DMA((72,)),
                pltpu.SemaphoreType.DMA((72,)),
            ],
            compiler_params=pltpu.CompilerParams(
                collective_id=0, has_side_effects=True, vmem_limit_bytes=67043328
            ),
        )(points, right_side, neighbours, leaf_interp, leaf_skeleton, node_skeleton, node_gain, transfer)

    in_specs = (
        P("leaf", None), P(None, "leaf"), P("leaf", None), P("leaf", None, None),
        P("leaf", None), P(), P(), P(),
    )
    out_specs = (P(None, "leaf"), P(None, "leaf"))
    return jax.shard_map(device, mesh=mesh, in_specs=in_specs, out_specs=out_specs, check_vma=False)
```

```python
import functools

import jax
import jax.numpy as jnp
from jax import lax
from jax.experimental import pallas as pl
from jax.experimental.pallas import tpu as pltpu
from jax.sharding import PartitionSpec as P

MESH = pl.DeviceIdType.MESH
F32 = jnp.float32
BF16 = jnp.bfloat16
I32 = jnp.int32

LEAF, SKEL, DIM, CLS = 512, 256, 128, 64
LV = 8
LEAVES = 1024
HALF = CLS // 2
OWN = 2 * LEAF
WIDE = (LV + 4) * LEAF


def split(x):
    high = x.astype(BF16)
    return high, (x - high.astype(F32)).astype(BF16)


def dot(a, b, ca=1, cb=0):
    return lax.dot_general(a, b, (((ca,), (cb,)), ((), ())), preferred_element_type=F32)


def times(stacked, high, low, cb=0):
    rows = stacked.shape[0] // 2
    both = dot(stacked, high, 1, cb)
    return both[:rows] + both[rows:] + dot(stacked[:rows], low, 1, cb)


def stack(x):
    return jnp.concatenate(split(x), axis=0)


def times_f32(a, b, cb=0):
    high, low = split(b)
    return times(stack(a), high, low, cb)


def norm_columns(x):
    half = -0.5 * jnp.sum(x * x, axis=1, keepdims=True)
    half = jnp.broadcast_to(half, x.shape)
    first = half.astype(BF16).astype(F32)
    rest = half - first
    second = rest.astype(BF16).astype(F32)
    third = rest - second
    lane = lax.broadcasted_iota(I32, x.shape, 1)
    parts = jnp.where(lane % 3 == 0, first, jnp.where(lane % 3 == 1, second, third))
    ones = jnp.ones_like(parts)
    zero = jnp.zeros_like(parts)
    low = jnp.where(lane < 3, ones, jnp.where(lane < 6, parts, zero))
    high = jnp.where(lane < 3, parts, jnp.where(lane < 6, ones, zero))
    return low.astype(BF16), high.astype(BF16)


def exponent(a_hl, a_n1, b_hl, b_n2):
    a_h = a_hl[:, :DIM]
    b_h, b_l = b_hl[:, :DIM], b_hl[:, DIM:]
    first = dot(a_hl, jnp.concatenate([b_h, b_h], axis=1), 1, 1)
    second = dot(
        jnp.concatenate([a_h, a_n1], axis=1), jnp.concatenate([b_l, b_n2], axis=1), 1, 1
    )
    return first + second


def transposed(top):
    return jnp.concatenate([top, jnp.zeros_like(top)], axis=0).T


def solve(matrix, target):
    work = jnp.concatenate([matrix, target], axis=1)
    row_id = lax.broadcasted_iota(I32, work.shape, 0)
    block = 4
    for start in range(0, CLS, block):
        columns = [
            jnp.broadcast_to(work[:, start + i : start + i + 1], work.shape) for i in range(block)
        ]
        for i in range(block):
            k = start + i
            here = row_id == k
            inverse = 1.0 / columns[i][k : k + 1, :]
            pivot = work[k : k + 1, :] * inverse
            work = jnp.where(here, pivot, work - columns[i] * pivot)
            for j in range(i + 1, block):
                entry = columns[j][k : k + 1, :] * inverse
                columns[j] = jnp.where(here, entry, columns[j] - columns[i] * entry)
    return work


def body(
    points, right_side, neighbours, leaf_interp, leaf_skeleton, node_skeleton, node_gain, transfer,
    x_out, r_out, d_out, a_out, c_out,
    xe, xhl, n1, n2, tile_h, tile_l, be, ye, near, dirn, vs, itp, tra, gw, nw, lsk, idx_rows, idx_cols,
    fh, fl, s_r0, s_q, w_r0, w_q, u4, ar_r0, ar_q, coef,
    local_sem, send_sem, recv_sem,
):
    me = lax.axis_index("leaf")
    core = me % 2
    chip = me // 2
    left = (me + 127) % 128
    right = (me + 1) % 128
    partner = me + 1 - 2 * core

    def peer(axis, s):
        stride = (2, 8, 32)[axis]
        at = (me // stride) % 4
        if s == 1:
            other = at + 1 - 2 * (at % 2)
        elif s == 2:
            other = at + 2 - 4 * (at // 2)
        else:
            other = 3 - at
        return me + (other - at) * stride

    def xor(n, s):
        if s == 1:
            return n + 1 - 2 * (n % 2)
        if s == 2:
            return n + 2 - 4 * ((n // 2) % 2)
        return xor(xor(n, 1), 2)

    loads = []

    def load(src, dst):
        copy = pltpu.make_async_copy(src, dst, local_sem.at[len(loads)])
        copy.start()
        loads.append(copy)
        return copy

    own_rows = pl.ds(OWN, LV * LEAF)
    load_points = load(points, xe.at[own_rows, :])
    load_small = [load(leaf_skeleton, lsk)]

    def gain_row(level):
        return 2 * LEAVES - 2 * (LEAVES >> level)

    def skel_row(level):
        return LEAVES - 2 * (LEAVES >> level)

    gain_node = [me * 8, me * 4, me * 2, me, me // 2, me // 4, me // 8, me // 16, me // 32]
    for level in range(9):
        if level < 8:
            at = pl.multiple_of(gain_row(level) + (gain_node[level] // 8) * 8, 8)
            load_small.append(load(node_gain.at[pl.ds(at, 8), :], gw.at[level]))
        else:
            load_small.append(load(node_gain.at[pl.ds(2040, 6), :], gw.at[level, pl.ds(0, 6), :]))
    skel_node = [None, me * 4, me * 2, me, me // 2, me // 4, me // 8, me // 16]
    for level in range(1, 9):
        if level < 8:
            at = pl.multiple_of(skel_row(level) + (skel_node[level] // 8) * 8, 8)
            load_small.append(load(node_skeleton.at[pl.ds(at, 8), :], nw.at[level]))
        else:
            load_small.append(load(node_skeleton.at[pl.ds(1016, 6), :], nw.at[level, pl.ds(0, 6), :]))
    load_b = load(right_side, be.at[:, own_rows])
    load_itp = load(leaf_interp, itp)
    load_tra = load(transfer, tra)

    peers = [partner, left, right] + [peer(a, s) for a in range(3) for s in (1, 2, 3)]
    barrier = pltpu.get_barrier_semaphore()
    for other in peers:
        pl.semaphore_signal(barrier, inc=1, device_id=(other,), device_id_type=MESH)

    sent = []

    def send(src, dst, device):
        k = len(sent)
        copy = pltpu.make_async_remote_copy(
            src_ref=src, dst_ref=dst, send_sem=send_sem.at[k], recv_sem=recv_sem.at[k],
            device_id=(device,), device_id_type=MESH,
        )
        copy.start()
        sent.append(copy)
        return copy

    def send_quad(buf, index, axis):
        return [send(buf.at[index, 0], buf.at[index, s], peer(axis, s)) for s in (1, 2, 3)]

    def arrive(copies):
        for copy in copies:
            copy.wait_recv()

    first, last = pl.ds(OWN, OWN), pl.ds(OWN + (LV - 2) * LEAF, OWN)
    head, tail = pl.ds(0, OWN), pl.ds(OWN + LV * LEAF, OWN)

    def halo_rows(ref):
        return [send(ref.at[first, :], ref.at[tail, :], left), send(ref.at[last, :], ref.at[head, :], right)]

    def halo_columns(ref):
        return [send(ref.at[:, first], ref.at[:, tail], left), send(ref.at[:, last], ref.at[:, head], right)]

    def split_rows(e):
        rows = pl.ds(pl.multiple_of(e * LEAF, LEAF), LEAF)
        xhl[rows, :] = jnp.concatenate(split(xe[rows, :]), axis=1)

    def prepare(e):
        rows = pl.ds(pl.multiple_of(e * LEAF, LEAF), LEAF)
        a, b = norm_columns(xe[rows, :])
        n1[rows, :] = a
        n2[rows, :] = b

    def split_columns(src, e):
        cols = pl.ds(pl.multiple_of(e * LEAF, LEAF), LEAF)
        high, low = split(src[:, cols])
        vs[pl.ds(0, CLS), cols] = high
        vs[pl.ds(CLS, CLS), cols] = low

    def loop(start, stop, f):
        def step(i, carry):
            f(i)
            return carry

        lax.fori_loop(start, stop, step, 0)

    load_points.wait()
    loop(2, 10, split_rows)

    def loop2(start, stop, f):
        def step(i, carry):
            f(start + 2 * i)
            f(start + 2 * i + 1)
            return carry

        lax.fori_loop(0, (stop - start) // 2, step, 0)

    for copy in load_small:
        copy.wait()
    idx_rows[...] = jnp.zeros_like(idx_rows)
    idx_rows[pl.ds(0, 8), :] = lsk[...].astype(F32)

    def put_index(slot, level, row, parity):
        index = nw[level, pl.ds(row, 1), :] + 256 * parity
        index = jnp.where(index >= 512, index - 512, index)
        idx_rows[pl.ds(slot, 1), :] = index.astype(F32)

    for i in range(4):
        put_index(8 + i, 1, (me * 4) % 8 + i, 0)
    for i in range(2):
        put_index(12 + i, 2, (me * 2) % 8 + i, 0)
    put_index(14, 3, me % 8, 0)
    put_index(15, 4, (me // 2) % 8, me % 2)
    n4, n6, n8 = me // 2, me // 8, me // 32
    quad_level = (4, 6, 8)
    quad_node = (n4, n6, n8)
    for q in range(3):
        level, node = quad_level[q], quad_node[q]
        parent = node // 2
        lv = min(level + 1, 8)
        base = 4 if level == 8 else 0
        put_index(16 + 3 * q, lv, base + parent % 8, node % 2)
        put_index(17 + 3 * q, lv, base + xor(parent, 1) % 8, node % 2)
        if q < 2:
            grand = parent // 2
            put_index(18 + 3 * q, level + 2, grand % 8, parent % 2)
    idx_cols[...] = idx_rows[...].T.astype(I32)

    def pick(slot, rows_hl):
        lane = lax.broadcasted_iota(I32, (SKEL, 2 * SKEL), 1)
        chosen = jnp.broadcast_to(idx_cols[:, slot : slot + 1], (SKEL, 2 * SKEL))
        one_hot = jnp.where(lane == chosen, 1.0, 0.0).astype(BF16)
        return dot(one_hot, rows_hl).astype(BF16)

    def joined(hl):
        return hl[:, :DIM].astype(F32) + hl[:, DIM:].astype(F32)

    def far_tile(slot, sibling_hl, own_hl):
        a1, _ = norm_columns(joined(sibling_hl))
        _, b2 = norm_columns(joined(own_hl))
        high, low = split(jnp.exp(exponent(sibling_hl, a1, own_hl, b2)))
        fh[slot] = high
        fl[slot] = low

    skel = [pick(j, xhl[pl.ds(OWN + j * LEAF, LEAF), :]) for j in range(LV)]
    index = 8
    pairs = []
    while len(skel) > 1:
        parents = []
        for i in range(len(skel) // 2):
            pairs.append((skel[2 * i + 1], skel[2 * i]))
            parents.append(pick(index, jnp.concatenate(skel[2 * i : 2 * i + 2], axis=0)))
            index += 1
        skel = parents
    skel3 = skel[0]
    s_r0[0] = joined(skel3)
    pl.semaphore_wait(barrier, len(peers))
    copy_s = [send(s_r0.at[0], s_r0.at[1], partner)]
    halo_x = halo_rows(xe)

    def gain(level, node):
        row = node % 8
        return gw[level, pl.ds(row, 1), :]

    class Tree:
        pass

    def up_local(it):
        t = Tree()
        t.levels = []
        rows = []
        for j in range(LV):
            v = vs[:, pl.ds(OWN + j * LEAF, LEAF)]
            high, low = split(itp[j])
            rows.append(times(v, high, low))
        for level in range(3):
            t.levels.append(rows)
            count = len(rows)
            lefts = jnp.concatenate(
                [rows[n] * gain(level, me * count + n) for n in range(0, count, 2)], axis=0
            )
            rights = jnp.concatenate(
                [rows[n] * gain(level, me * count + n) for n in range(1, count, 2)], axis=0
            )
            joint = times_f32(lefts, tra[level, 0]) + times_f32(rights, tra[level, 1])
            rows = [joint[n * CLS : (n + 1) * CLS] for n in range(count // 2)]
        w_r0[it, 0] = rows[0]
        t.copies = [send(w_r0.at[it, 0], w_r0.at[it, 1], partner)]
        return t

    my_half = pl.ds(pl.multiple_of(core * HALF, HALF), HALF)

    def up_core(it, t):
        arrive(t.copies)
        own = w_r0[it, 0, my_half, :] * gain(3, me)
        sib = w_r0[it, 1, my_half, :] * gain(3, partner)
        w_q[it * 3, 0] = times_f32(own, tra[3, core]) + times_f32(sib, tra[3, 1 - core])
        t.copies = send_quad(w_q, it * 3, 0)
        t.sib = {}

    def up_quad(it, t, q):
        arrive(t.copies)
        level, node = quad_level[q], quad_node[q]
        parity = node % 2
        four = [w_q[it * 3 + q, s] for s in range(4)]
        t.sib[level] = four[1]
        if q == 2:
            a = four[2] * gain(level, xor(node, 2))
            b = four[3] * gain(level, xor(node, 3))
            t.sib[level + 1] = times_f32(a, tra[level, parity]) + times_f32(b, tra[level, 1 - parity])
            return
        a = jnp.concatenate([four[0] * gain(level, node), four[2] * gain(level, xor(node, 2))], axis=0)
        b = jnp.concatenate(
            [four[1] * gain(level, xor(node, 1)), four[3] * gain(level, xor(node, 3))], axis=0
        )
        two = times_f32(a, tra[level, parity]) + times_f32(b, tra[level, 1 - parity])
        t.sib[level + 1] = two[HALF:]
        parent = node // 2
        parity = parent % 2
        a = two[:HALF] * gain(level + 1, parent)
        b = two[HALF:] * gain(level + 1, xor(parent, 1))
        w_q[it * 3 + q + 1, 0] = times_f32(a, tra[level + 1, parity]) + times_f32(
            b, tra[level + 1, 1 - parity]
        )
        t.copies = send_quad(w_q, it * 3 + q + 1, q + 1)

    def down_top(it, t):
        pot = times(stack(t.sib[9]), fh[13], fl[13])
        for level in range(8, 3, -1):
            node = me // (1 << (level - 3))
            pot = times_f32(pot, tra[level, node % 2], 1) * gain(level, node)
            pot = pot + times(stack(t.sib[level]), fh[level + 4], fl[level + 4])
        u4[it, my_half, :] = pot
        t.copies = [send(u4.at[it, my_half, :], u4.at[it, my_half, :], partner)]

    def down_device(it, t):
        arrive(t.copies)
        pot = times_f32(u4[it], tra[3, core], 1) * gain(3, me)
        t.top = pot + times(stack(w_r0[it, 1]), fh[7], fl[7])

    def tree_gram(t):
        total = None
        slot = 0
        for level in range(3):
            rows = t.levels[level]
            for i in range(len(rows) // 2):
                part = times(stack(rows[2 * i + 1]), fh[slot], fl[slot])
                part = times_f32(rows[2 * i], part, 1)
                total = part if total is None else total + part
                slot += 1
        return total

    def down_local(it, t, store):
        pot = t.top
        slot = 7
        for level in (2, 1, 0):
            rows = t.levels[level]
            count = len(rows)
            slot -= count // 2
            stacked = stack(pot)
            out = []
            lefts = times(stacked, *split(tra[level, 0]), 1)
            rights = times(stacked, *split(tra[level, 1]), 1)
            for n in range(count):
                part = (lefts, rights)[n % 2][(n // 2) * CLS : (n // 2 + 1) * CLS]
                part = part * gain(level, me * count + n)
                other = stack(rows[n + 1 - 2 * (n % 2)])
                f = slot + n // 2
                out.append(part + times(other, fh[f], fl[f], n % 2))
            pot = jnp.concatenate(out, axis=0)
        for j in range(LV):
            high, low = split(itp[j])
            store(j, times(stack(pot[j * CLS : (j + 1) * CLS]), high, low, 1))

    my_points = pl.ds(pl.multiple_of(core * 128, 128), 128)

    def send_skel(q):
        return [
            send(s_q.at[q, 0, my_points, :], s_q.at[q, s, my_points, :], peer(q, s)) for s in (1, 2, 3)
        ]

    def forward_skel(q, copies):
        arrive(copies)
        part = s_q.at[q, pl.ds(1, 3), my_points, :]
        return [send(part, part, partner)]

    def skel_core():
        arrive(copy_s)
        other = jnp.concatenate(split(s_r0[1]), axis=1)
        own = pick(15, jnp.concatenate([skel3, other], axis=0))
        s_q[0, 0] = joined(own)
        return (own, [(7, other, skel3)], send_skel(0))

    def skel_quad(q, own, copies):
        arrive(copies)
        s1, s2, s3 = [jnp.concatenate(split(s_q[q, s]), axis=1) for s in (1, 2, 3)]
        mine = pick(16 + 3 * q, jnp.concatenate([own, s1], axis=0))
        theirs = pick(17 + 3 * q, jnp.concatenate([s2, s3], axis=0))
        tiles = [(8 + 2 * q, s1, own), (9 + 2 * q, theirs, mine)]
        if q == 2:
            return None, tiles, None
        up = pick(18 + 3 * q, jnp.concatenate([mine, theirs], axis=0))
        s_q[q + 1, 0] = joined(up)
        return up, tiles, send_skel(q + 1)

    def far_tiles(tiles):
        for tile in tiles:
            far_tile(*tile)

    def build(t):
        e = (t + 6) // 3
        k = (t + 6) % 3
        rows = pl.ds(pl.multiple_of(e * LEAF, LEAF), LEAF)
        cols = pl.ds(pl.multiple_of((e + k) * LEAF, LEAF), LEAF)
        if isinstance(t, int):
            flag = neighbours[e - 2, 2 + k] if e >= 2 else neighbours[e + k - 2, 2 - k]
        else:
            flag = neighbours[e - 2, 2 + k]
        mask = jnp.where(flag >= 0, 1.0, 0.0).astype(F32)
        high, low = split(jnp.exp(exponent(xhl[rows, :], n1[rows, :], xhl[cols, :], n2[cols, :])) * mask)
        tile_h[t + 4] = high
        tile_l[t + 4] = low

    def near_target(j):
        total = None
        for o in (0, -1, -2):
            cols = pl.ds(pl.multiple_of((j + 2 + o) * LEAF, LEAF), LEAF)
            t = 3 * (j + o) - o
            part = times(vs[:, cols], tile_h[t + 4], tile_l[t + 4])
            total = part if total is None else total + part
        turned = None
        for o in (1, 2):
            cols = pl.ds(pl.multiple_of((j + 2 + o) * LEAF, LEAF), LEAF)
            t = 3 * j + o
            part = dot(tile_h[t + 4], vs[:, cols], 1, 1) + dot(tile_l[t + 4], vs[:, cols], 1, 1)
            turned = part if turned is None else turned + part
        turned = turned.T
        return total + (turned[:CLS] + turned[CLS:])

    def gram(pairs):
        sums = None
        for j in range(LV):
            stacks = {}

            def get(ref, at):
                if id(ref) not in stacks:
                    stacks[id(ref)] = stack(ref[:, pl.ds(at + j * LEAF, LEAF)])
                return stacks[id(ref)]

            parts = []
            for a, a0, b, b0 in pairs:
                bs = get(b, b0)
                parts.append(times(get(a, a0), bs[:CLS], bs[CLS:], 1))
            sums = parts if sums is None else [s + p for s, p in zip(sums, parts)]
        return sums

    class Sum:
        pass

    def sum_start(index, value):
        r = Sum()
        rows = value.shape[0]
        r.rows, r.index = pl.ds(0, rows), index
        ar_r0[index, 0, r.rows, :] = value
        r.copies = [send(ar_r0.at[index, 0, r.rows, :], ar_r0.at[index, 1, r.rows, :], partner)]
        return r

    def sum_step(r, stage):
        arrive(r.copies)
        if stage == 0:
            value = ar_r0[r.index, 0, r.rows, :] + ar_r0[r.index, 1, r.rows, :]
        else:
            at = r.index * 3 + stage - 1
            value = (ar_q[at, 0, r.rows, :] + ar_q[at, 1, r.rows, :]) + (
                ar_q[at, 2, r.rows, :] + ar_q[at, 3, r.rows, :]
            )
        if stage < 3:
            at = r.index * 3 + stage
            ar_q[at, 0, r.rows, :] = value
            r.copies = [
                send(ar_q.at[at, 0, r.rows, :], ar_q.at[at, s, r.rows, :], peer(stage, s)) for s in (1, 2, 3)
            ]
        return value

    def folded(m):
        return jnp.concatenate([m[:HALF], m[HALF:]], axis=1)

    def unfolded(m):
        return jnp.concatenate([m[:, :CLS], m[:, CLS:]], axis=0)

    def square_t(m):
        return jnp.concatenate([m, jnp.zeros_like(m)], axis=1)

    def low_pairs_t(m):
        return transposed(square_t(m))[:CLS, :CLS]

    def sym(m):
        return 0.5 * (m + transposed(square_t(m))[:CLS, :CLS])

    def inverse_of(m):
        row = lax.broadcasted_iota(I32, (CLS, CLS), 0)
        col = lax.broadcasted_iota(I32, (CLS, CLS), 1)
        return solve(m, jnp.where(row == col, 1.0, 0.0).astype(F32))[:, CLS:]

    loop2(2, 10, prepare)
    far_tiles([(i, *pair) for i, pair in enumerate(pairs)])
    loop2(0, 2, build)
    own4, tiles3, copy_s = skel_core()
    load_b.wait()

    def split_b(e):
        split_columns(be, e)

    loop(2, 10, split_b)
    load_itp.wait()
    load_tra.wait()
    t0 = up_local(0)
    sum0 = sum_start(0, folded(gram([(be, OWN, be, OWN)])[0]))
    loop2(2, 6, build)
    up_core(0, t0)
    sum_step(sum0, 0)
    far_tiles(tiles3)
    loop2(6, 10, build)
    copy_s = forward_skel(0, copy_s)
    loop2(10, 12, build)
    own6, tiles4, copy_s = skel_quad(0, own4, copy_s)
    up_quad(0, t0, 0)
    sum_step(sum0, 1)
    far_tiles(tiles4)
    loop2(12, 20, build)
    copy_s = forward_skel(1, copy_s)
    up_quad(0, t0, 1)
    sum_step(sum0, 2)
    own8, tiles6, copy_s = skel_quad(1, own6, copy_s)
    halo_b = halo_columns(be)
    far_tiles(tiles6)
    arrive(halo_x)

    def halo_setup(e):
        split_rows(e)
        prepare(e)

    loop(0, 2, halo_setup)
    loop(10, 12, halo_setup)
    loop2(20, 24, build)
    copy_s = forward_skel(2, copy_s)
    arrive(halo_b)
    for t in (-4, -2, -1):
        build(t)
    loop(0, 2, split_b)
    loop(10, 12, split_b)
    up_quad(0, t0, 2)
    m0 = unfolded(sum_step(sum0, 3))
    _, tiles8, _ = skel_quad(2, own8, copy_s)
    far_tiles(tiles8)
    down_top(0, t0)

    def first_near(j):
        cols = pl.ds(pl.multiple_of((j + 2) * LEAF, LEAF), LEAF)
        ye[:, cols] = be[:, cols] + near_target(j)

    loop2(0, LV, first_near)
    down_device(0, t0)

    def store_first(j, far):
        cols = pl.ds(OWN + j * LEAF, LEAF)
        ye[:, cols] = ye[:, cols] + far

    down_local(0, t0, store_first)

    def split_y(e):
        split_columns(ye, e)

    loop(2, 10, split_y)
    t1 = up_local(1)
    sum1 = sum_start(1, jnp.concatenate(gram([(be, OWN, ye, OWN), (ye, OWN, ye, OWN)]), axis=1))

    def second_near(j):
        cols = pl.ds(pl.multiple_of(j * LEAF, LEAF), LEAF)
        near[:, cols] = near_target(j)

    up_core(1, t1)
    sum_step(sum1, 0)
    low_pairs = tree_gram(t1)
    loop2(2, 6, second_near)
    up_quad(1, t1, 0)
    sum_step(sum1, 1)
    halo_y = halo_columns(ye)
    inverse0 = inverse_of(sym(m0))
    up_quad(1, t1, 1)
    sum_step(sum1, 2)
    arrive(halo_y)
    loop(0, 2, split_y)
    loop(10, 12, split_y)
    loop2(0, 2, second_near)
    loop2(6, 8, second_near)
    near_gram = gram([(ye, OWN, near, 0)])[0]
    up_quad(1, t1, 2)
    down_top(1, t1)
    moments = sum_step(sum1, 3)
    down_device(1, t1)
    bends = near_gram + low_pairs + low_pairs_t(low_pairs) + times_f32(w_r0[1, 0], t1.top, 1)
    curve = sum_start(2, folded(bends))

    def store_second(j, far):
        cols = pl.ds(j * LEAF, LEAF)
        near[:, cols] = near[:, cols] + far + ye[:, pl.ds(OWN + j * LEAF, LEAF)]

    m0 = sym(m0)
    m1 = moments[:, :CLS]
    m2 = moments[:, CLS:]
    step = solve(sym(m1), m0)
    sum_step(curve, 0)
    alpha = step[:, CLS:]
    alpha_t = transposed(step)[CLS:, :CLS]
    cross = times_f32(m1, alpha)
    new = m0 - 2.0 * sym(cross) + sym(times_f32(times_f32(alpha_t, m2), alpha))
    beta = times_f32(inverse0, new)
    beta_t = low_pairs_t(beta)
    row = lax.broadcasted_iota(I32, (CLS, CLS), 0)
    col = lax.broadcasted_iota(I32, (CLS, CLS), 1)
    unit = jnp.where(row == col, 1.0, 0.0)
    plus = unit + beta
    plus_t = unit + beta_t
    down_local(1, t1, store_second)
    sum_step(curve, 1)

    alpha_s = stack(alpha_t)
    plus_s = stack(plus_t)

    def mix(matrix_s, x):
        high, low = split(x)
        return times(matrix_s, high, low)

    for copy in halo_b + halo_y:
        copy.wait_send()

    def update(j):
        cols = pl.ds(pl.multiple_of(j * 2 * LEAF, LEAF), 2 * LEAF)
        wide = pl.ds(pl.multiple_of((j + 1) * 2 * LEAF, LEAF), 2 * LEAF)
        old, image = be[:, wide], ye[:, wide]
        start = mix(alpha_s, image)
        dirn[:, cols] = mix(plus_s, old) - start
        near[:, cols] = mix(plus_s, image) - mix(alpha_s, near[:, cols])
        be[:, wide] = mix(alpha_s, old)
        ye[:, wide] = old - start

    loop(0, LV // 2, update)
    outs = [
        load(be.at[:, own_rows], x_out), load(ye.at[:, own_rows], r_out),
        load(dirn, d_out), load(near, a_out),
    ]
    sum_step(curve, 2)
    known = times_f32(times_f32(plus_t, m1), plus) - 2.0 * sym(times_f32(times_f32(plus_t, m2), alpha))
    known = known + times_f32(times_f32(alpha_t, m2), alpha)
    bends = unfolded(sum_step(curve, 3))
    curvature = sym(known + times_f32(times_f32(alpha_t, bends), alpha))
    coef[...] = transposed(solve(curvature, new))[CLS:, :]
    outs.append(load(coef, c_out))
    for copy in outs:
        copy.wait()
    for copy in sent:
        if not any(copy is done for done in halo_b + halo_y):
            copy.wait_send()


def finish(coef, x0, r1, direction, image, x_out, r_out):
    last_s = stack(coef[:, :CLS])
    high, low = split(direction[...])
    x_out[...] = x0[...] + times(last_s, high, low)
    high, low = split(image[...])
    r_out[...] = r1[...] - times(last_s, high, low)


def solution(mesh):
    any_space = pl.BlockSpec(memory_space=pl.ANY)
    vmem = pltpu.VMEM

    def device(points, right_side, neighbours, leaf_interp, leaf_skeleton, node_skeleton, node_gain, transfer):
        out = jax.ShapeDtypeStruct(right_side.shape, F32)
        x0, r1, direction, image, coef = pl.pallas_call(
            body,
            out_shape=(out, out, out, out, jax.ShapeDtypeStruct((CLS, 128), F32)),
            in_specs=[
                any_space, any_space, pl.BlockSpec(memory_space=pltpu.SMEM), any_space,
                any_space, any_space, any_space, any_space,
            ],
            out_specs=(any_space,) * 5,
            scratch_shapes=[
                vmem((WIDE, DIM), F32),
                vmem((WIDE, 2 * DIM), BF16),
                vmem((WIDE, DIM), BF16),
                vmem((WIDE, DIM), BF16),
                vmem((28, LEAF, LEAF), BF16),
                vmem((28, LEAF, LEAF), BF16),
                vmem((CLS, WIDE), F32),
                vmem((CLS, WIDE), F32),
                vmem((CLS, LV * LEAF), F32),
                vmem((CLS, LV * LEAF), F32),
                vmem((2 * CLS, WIDE), BF16),
                vmem((LV, LEAF, SKEL), F32),
                vmem((9, 2, SKEL, SKEL), F32),
                vmem((9, 8, SKEL), F32),
                vmem((9, 8, SKEL), I32),
                vmem((LV, SKEL), I32),
                vmem((128, SKEL), F32),
                vmem((SKEL, 128), I32),
                vmem((14, SKEL, SKEL), BF16),
                vmem((14, SKEL, SKEL), BF16),
                vmem((2, SKEL, DIM), F32),
                vmem((3, 4, SKEL, DIM), F32),
                vmem((2, 2, CLS, SKEL), F32),
                vmem((6, 4, HALF, SKEL), F32),
                vmem((2, CLS, SKEL), F32),
                vmem((3, 2, CLS, 128), F32),
                vmem((9, 4, CLS, 128), F32),
                vmem((CLS, 128), F32),
                pltpu.SemaphoreType.DMA((28,)),
                pltpu.SemaphoreType.DMA((72,)),
                pltpu.SemaphoreType.DMA((72,)),
            ],
            compiler_params=pltpu.CompilerParams(
                collective_id=0, has_side_effects=True, vmem_limit_bytes=67043328
            ),
        )(points, right_side, neighbours, leaf_interp, leaf_skeleton, node_skeleton, node_gain, transfer)
        block = pl.BlockSpec((CLS, 2 * LEAF), lambda j: (0, j))
        return pl.pallas_call(
            finish,
            grid=(LV // 2,),
            out_shape=(out, out),
            in_specs=[pl.BlockSpec((CLS, 128), lambda j: (0, 0)), block, block, block, block],
            out_specs=(block, block),
        )(coef, x0, r1, direction, image)

    in_specs = (
        P("leaf", None), P(None, "leaf"), P("leaf", None), P("leaf", None, None),
        P("leaf", None), P(), P(), P(),
    )
    out_specs = (P(None, "leaf"), P(None, "leaf"))
    return jax.shard_map(device, mesh=mesh, in_specs=in_specs, out_specs=out_specs, check_vma=False)
```

```python
import functools

import jax
import jax.numpy as jnp
from jax import lax
from jax.experimental import pallas as pl
from jax.experimental.pallas import tpu as pltpu
from jax.sharding import PartitionSpec as P

MESH = pl.DeviceIdType.MESH
F32 = jnp.float32
BF16 = jnp.bfloat16
I32 = jnp.int32

LEAF, SKEL, DIM, CLS = 512, 256, 128, 64
LV = 8
LEAVES = 1024
HALF = CLS // 2
OWN = 2 * LEAF
WIDE = (LV + 4) * LEAF


def split(x):
    high = x.astype(BF16)
    return high, (x - high.astype(F32)).astype(BF16)


def dot(a, b, ca=1, cb=0):
    return lax.dot_general(a, b, (((ca,), (cb,)), ((), ())), preferred_element_type=F32)


def times(stacked, high, low, cb=0):
    rows = stacked.shape[0] // 2
    both = dot(stacked, high, 1, cb)
    return both[:rows] + both[rows:] + dot(stacked[:rows], low, 1, cb)


def stack(x):
    return jnp.concatenate(split(x), axis=0)


def times_f32(a, b, cb=0):
    high, low = split(b)
    return times(stack(a), high, low, cb)


def norm_columns(x):
    half = -0.5 * jnp.sum(x * x, axis=1, keepdims=True)
    half = jnp.broadcast_to(half, x.shape)
    first = half.astype(BF16).astype(F32)
    rest = half - first
    second = rest.astype(BF16).astype(F32)
    third = rest - second
    lane = lax.broadcasted_iota(I32, x.shape, 1)
    parts = jnp.where(lane % 3 == 0, first, jnp.where(lane % 3 == 1, second, third))
    ones = jnp.ones_like(parts)
    zero = jnp.zeros_like(parts)
    low = jnp.where(lane < 3, ones, jnp.where(lane < 6, parts, zero))
    high = jnp.where(lane < 3, parts, jnp.where(lane < 6, ones, zero))
    return low.astype(BF16), high.astype(BF16)


def exponent(a_hl, a_n1, b_hl, b_n2):
    a_h = a_hl[:, :DIM]
    b_h, b_l = b_hl[:, :DIM], b_hl[:, DIM:]
    first = dot(a_hl, jnp.concatenate([b_h, b_h], axis=1), 1, 1)
    second = dot(
        jnp.concatenate([a_h, a_n1], axis=1), jnp.concatenate([b_l, b_n2], axis=1), 1, 1
    )
    return first + second


def transposed(top):
    return jnp.concatenate([top, jnp.zeros_like(top)], axis=0).T


def solve(matrix, target):
    work = jnp.concatenate([matrix, target], axis=1)
    row_id = lax.broadcasted_iota(I32, work.shape, 0)
    block = 4
    for start in range(0, CLS, block):
        columns = [
            jnp.broadcast_to(work[:, start + i : start + i + 1], work.shape) for i in range(block)
        ]
        for i in range(block):
            k = start + i
            here = row_id == k
            inverse = 1.0 / columns[i][k : k + 1, :]
            pivot = work[k : k + 1, :] * inverse
            work = jnp.where(here, pivot, work - columns[i] * pivot)
            for j in range(i + 1, block):
                entry = columns[j][k : k + 1, :] * inverse
                columns[j] = jnp.where(here, entry, columns[j] - columns[i] * entry)
    return work


def body(
    points, right_side, neighbours, leaf_interp, leaf_skeleton, node_skeleton, node_gain, transfer,
    x_out, r_out, d_out, a_out, c_out,
    xe, xhl, n1, n2, tile_h, tile_l, be, ye, near, vs, itp, tra, gw, nw, lsk, idx_rows, idx_cols,
    fh, fl, s_r0, s_q, w_r0, w_q, u4, ar_r0, ar_q, coef,
    local_sem, send_sem, recv_sem,
):
    me = lax.axis_index("leaf")
    core = me % 2
    chip = me // 2
    left = (me + 127) % 128
    right = (me + 1) % 128
    partner = me + 1 - 2 * core

    def peer(axis, s):
        stride = (2, 8, 32)[axis]
        at = (me // stride) % 4
        if s == 1:
            other = at + 1 - 2 * (at % 2)
        elif s == 2:
            other = at + 2 - 4 * (at // 2)
        else:
            other = 3 - at
        return me + (other - at) * stride

    def xor(n, s):
        if s == 1:
            return n + 1 - 2 * (n % 2)
        if s == 2:
            return n + 2 - 4 * ((n // 2) % 2)
        return xor(xor(n, 1), 2)

    loads = []

    def load(src, dst):
        copy = pltpu.make_async_copy(src, dst, local_sem.at[len(loads)])
        copy.start()
        loads.append(copy)
        return copy

    own_rows = pl.ds(OWN, LV * LEAF)
    load_points = load(points, xe.at[own_rows, :])
    load_small = [load(leaf_skeleton, lsk)]

    def gain_row(level):
        return 2 * LEAVES - 2 * (LEAVES >> level)

    def skel_row(level):
        return LEAVES - 2 * (LEAVES >> level)

    gain_node = [me * 8, me * 4, me * 2, me, me // 2, me // 4, me // 8, me // 16, me // 32]
    for level in range(9):
        if level < 8:
            at = pl.multiple_of(gain_row(level) + (gain_node[level] // 8) * 8, 8)
            load_small.append(load(node_gain.at[pl.ds(at, 8), :], gw.at[level]))
        else:
            load_small.append(load(node_gain.at[pl.ds(2040, 6), :], gw.at[level, pl.ds(0, 6), :]))
    skel_node = [None, me * 4, me * 2, me, me // 2, me // 4, me // 8, me // 16]
    for level in range(1, 9):
        if level < 8:
            at = pl.multiple_of(skel_row(level) + (skel_node[level] // 8) * 8, 8)
            load_small.append(load(node_skeleton.at[pl.ds(at, 8), :], nw.at[level]))
        else:
            load_small.append(load(node_skeleton.at[pl.ds(1016, 6), :], nw.at[level, pl.ds(0, 6), :]))
    load_b = load(right_side, be.at[:, own_rows])
    load_itp = load(leaf_interp, itp)
    load_tra = load(transfer, tra)

    peers = [partner, left, right] + [peer(a, s) for a in range(3) for s in (1, 2, 3)]
    barrier = pltpu.get_barrier_semaphore()
    for other in peers:
        pl.semaphore_signal(barrier, inc=1, device_id=(other,), device_id_type=MESH)

    sent = []

    def send(src, dst, device):
        k = len(sent)
        copy = pltpu.make_async_remote_copy(
            src_ref=src, dst_ref=dst, send_sem=send_sem.at[k], recv_sem=recv_sem.at[k],
            device_id=(device,), device_id_type=MESH,
        )
        copy.start()
        sent.append(copy)
        return copy

    def send_quad(buf, index, axis):
        return [send(buf.at[index, 0], buf.at[index, s], peer(axis, s)) for s in (1, 2, 3)]

    def arrive(copies):
        for copy in copies:
            copy.wait_recv()

    first, last = pl.ds(OWN, OWN), pl.ds(OWN + (LV - 2) * LEAF, OWN)
    head, tail = pl.ds(0, OWN), pl.ds(OWN + LV * LEAF, OWN)

    def halo_rows(ref):
        return [send(ref.at[first, :], ref.at[tail, :], left), send(ref.at[last, :], ref.at[head, :], right)]

    def halo_columns(ref):
        return [send(ref.at[:, first], ref.at[:, tail], left), send(ref.at[:, last], ref.at[:, head], right)]

    def split_rows(e):
        rows = pl.ds(pl.multiple_of(e * LEAF, LEAF), LEAF)
        xhl[rows, :] = jnp.concatenate(split(xe[rows, :]), axis=1)

    def prepare(e):
        rows = pl.ds(pl.multiple_of(e * LEAF, LEAF), LEAF)
        a, b = norm_columns(xe[rows, :])
        n1[rows, :] = a
        n2[rows, :] = b

    def split_columns(src, e):
        cols = pl.ds(pl.multiple_of(e * LEAF, LEAF), LEAF)
        high, low = split(src[:, cols])
        vs[pl.ds(0, CLS), cols] = high
        vs[pl.ds(CLS, CLS), cols] = low

    def loop(start, stop, f):
        def step(i, carry):
            f(i)
            return carry

        lax.fori_loop(start, stop, step, 0)

    load_points.wait()
    pl.semaphore_wait(barrier, len(peers))
    halo_x = halo_rows(xe)
    loop(2, 10, split_rows)

    def loop2(start, stop, f):
        def step(i, carry):
            f(start + 2 * i)
            f(start + 2 * i + 1)
            return carry

        lax.fori_loop(0, (stop - start) // 2, step, 0)

    for copy in load_small:
        copy.wait()
    idx_rows[...] = jnp.zeros_like(idx_rows)
    idx_rows[pl.ds(0, 8), :] = lsk[...].astype(F32)

    def put_index(slot, level, row, parity):
        index = nw[level, pl.ds(row, 1), :] + 256 * parity
        index = jnp.where(index >= 512, index - 512, index)
        idx_rows[pl.ds(slot, 1), :] = index.astype(F32)

    for i in range(4):
        put_index(8 + i, 1, (me * 4) % 8 + i, 0)
    for i in range(2):
        put_index(12 + i, 2, (me * 2) % 8 + i, 0)
    put_index(14, 3, me % 8, 0)
    put_index(15, 4, (me // 2) % 8, me % 2)
    n4, n6, n8 = me // 2, me // 8, me // 32
    quad_level = (4, 6, 8)
    quad_node = (n4, n6, n8)
    for q in range(3):
        level, node = quad_level[q], quad_node[q]
        parent = node // 2
        lv = min(level + 1, 8)
        base = 4 if level == 8 else 0
        put_index(16 + 3 * q, lv, base + parent % 8, node % 2)
        put_index(17 + 3 * q, lv, base + xor(parent, 1) % 8, node % 2)
        if q < 2:
            grand = parent // 2
            put_index(18 + 3 * q, level + 2, grand % 8, parent % 2)
    idx_cols[...] = idx_rows[...].T.astype(I32)

    def pick(slot, rows_hl):
        lane = lax.broadcasted_iota(I32, (SKEL, 2 * SKEL), 1)
        chosen = jnp.broadcast_to(idx_cols[:, slot : slot + 1], (SKEL, 2 * SKEL))
        one_hot = jnp.where(lane == chosen, 1.0, 0.0).astype(BF16)
        return dot(one_hot, rows_hl).astype(BF16)

    def joined(hl):
        return hl[:, :DIM].astype(F32) + hl[:, DIM:].astype(F32)

    def far_tile(slot, sibling_hl, own_hl):
        a1, _ = norm_columns(joined(sibling_hl))
        _, b2 = norm_columns(joined(own_hl))
        high, low = split(jnp.exp(exponent(sibling_hl, a1, own_hl, b2)))
        fh[slot] = high
        fl[slot] = low

    skel = [pick(j, xhl[pl.ds(OWN + j * LEAF, LEAF), :]) for j in range(LV)]
    index = 8
    pairs = []
    while len(skel) > 1:
        parents = []
        for i in range(len(skel) // 2):
            pairs.append((skel[2 * i + 1], skel[2 * i]))
            parents.append(pick(index, jnp.concatenate(skel[2 * i : 2 * i + 2], axis=0)))
            index += 1
        skel = parents
    skel3 = skel[0]
    s_r0[0] = joined(skel3)
    copy_s = [send(s_r0.at[0], s_r0.at[1], partner)]

    def gain(level, node):
        row = node % 8
        return gw[level, pl.ds(row, 1), :]

    class Tree:
        pass

    def up_local(it):
        t = Tree()
        t.levels = []
        rows = []
        for j in range(LV):
            v = vs[:, pl.ds(OWN + j * LEAF, LEAF)]
            high, low = split(itp[j])
            rows.append(times(v, high, low))
        for level in range(3):
            t.levels.append(rows)
            count = len(rows)
            lefts = jnp.concatenate(
                [rows[n] * gain(level, me * count + n) for n in range(0, count, 2)], axis=0
            )
            rights = jnp.concatenate(
                [rows[n] * gain(level, me * count + n) for n in range(1, count, 2)], axis=0
            )
            joint = times_f32(lefts, tra[level, 0]) + times_f32(rights, tra[level, 1])
            rows = [joint[n * CLS : (n + 1) * CLS] for n in range(count // 2)]
        w_r0[it, 0] = rows[0]
        t.copies = [send(w_r0.at[it, 0], w_r0.at[it, 1], partner)]
        return t

    my_half = pl.ds(pl.multiple_of(core * HALF, HALF), HALF)

    def up_core(it, t):
        arrive(t.copies)
        own = w_r0[it, 0, my_half, :] * gain(3, me)
        sib = w_r0[it, 1, my_half, :] * gain(3, partner)
        w_q[it * 3, 0] = times_f32(own, tra[3, core]) + times_f32(sib, tra[3, 1 - core])
        t.copies = send_quad(w_q, it * 3, 0)
        t.sib = {}

    def up_quad(it, t, q):
        arrive(t.copies)
        level, node = quad_level[q], quad_node[q]
        parity = node % 2
        four = [w_q[it * 3 + q, s] for s in range(4)]
        t.sib[level] = four[1]
        if q == 2:
            a = four[2] * gain(level, xor(node, 2))
            b = four[3] * gain(level, xor(node, 3))
            t.sib[level + 1] = times_f32(a, tra[level, parity]) + times_f32(b, tra[level, 1 - parity])
            return
        a = jnp.concatenate([four[0] * gain(level, node), four[2] * gain(level, xor(node, 2))], axis=0)
        b = jnp.concatenate(
            [four[1] * gain(level, xor(node, 1)), four[3] * gain(level, xor(node, 3))], axis=0
        )
        two = times_f32(a, tra[level, parity]) + times_f32(b, tra[level, 1 - parity])
        t.sib[level + 1] = two[HALF:]
        parent = node // 2
        parity = parent % 2
        a = two[:HALF] * gain(level + 1, parent)
        b = two[HALF:] * gain(level + 1, xor(parent, 1))
        w_q[it * 3 + q + 1, 0] = times_f32(a, tra[level + 1, parity]) + times_f32(
            b, tra[level + 1, 1 - parity]
        )
        t.copies = send_quad(w_q, it * 3 + q + 1, q + 1)

    def down_top(it, t):
        pot = times(stack(t.sib[9]), fh[13], fl[13])
        for level in range(8, 3, -1):
            node = me // (1 << (level - 3))
            pot = times_f32(pot, tra[level, node % 2], 1) * gain(level, node)
            pot = pot + times(stack(t.sib[level]), fh[level + 4], fl[level + 4])
        u4[it, my_half, :] = pot
        t.copies = [send(u4.at[it, my_half, :], u4.at[it, my_half, :], partner)]

    def down_device(it, t):
        arrive(t.copies)
        pot = times_f32(u4[it], tra[3, core], 1) * gain(3, me)
        t.top = pot + times(stack(w_r0[it, 1]), fh[7], fl[7])

    def tree_gram(t):
        total = None
        slot = 0
        for level in range(3):
            rows = t.levels[level]
            for i in range(len(rows) // 2):
                part = times(stack(rows[2 * i + 1]), fh[slot], fl[slot])
                part = times_f32(rows[2 * i], part, 1)
                total = part if total is None else total + part
                slot += 1
        return total

    def down_local(it, t, store):
        pot = t.top
        slot = 7
        for level in (2, 1, 0):
            rows = t.levels[level]
            count = len(rows)
            slot -= count // 2
            stacked = stack(pot)
            out = []
            lefts = times(stacked, *split(tra[level, 0]), 1)
            rights = times(stacked, *split(tra[level, 1]), 1)
            for n in range(count):
                part = (lefts, rights)[n % 2][(n // 2) * CLS : (n // 2 + 1) * CLS]
                part = part * gain(level, me * count + n)
                other = stack(rows[n + 1 - 2 * (n % 2)])
                f = slot + n // 2
                out.append(part + times(other, fh[f], fl[f], n % 2))
            pot = jnp.concatenate(out, axis=0)
        for j in range(LV):
            high, low = split(itp[j])
            store(j, times(stack(pot[j * CLS : (j + 1) * CLS]), high, low, 1))

    my_points = pl.ds(pl.multiple_of(core * 128, 128), 128)

    def send_skel(q):
        return [
            send(s_q.at[q, 0, my_points, :], s_q.at[q, s, my_points, :], peer(q, s)) for s in (1, 2, 3)
        ]

    def forward_skel(q, copies):
        arrive(copies)
        part = s_q.at[q, pl.ds(1, 3), my_points, :]
        return [send(part, part, partner)]

    def skel_core():
        arrive(copy_s)
        other = jnp.concatenate(split(s_r0[1]), axis=1)
        own = pick(15, jnp.concatenate([skel3, other], axis=0))
        s_q[0, 0] = joined(own)
        return (own, [(7, other, skel3)], send_skel(0))

    def skel_quad(q, own, copies):
        arrive(copies)
        s1, s2, s3 = [jnp.concatenate(split(s_q[q, s]), axis=1) for s in (1, 2, 3)]
        mine = pick(16 + 3 * q, jnp.concatenate([own, s1], axis=0))
        theirs = pick(17 + 3 * q, jnp.concatenate([s2, s3], axis=0))
        tiles = [(8 + 2 * q, s1, own), (9 + 2 * q, theirs, mine)]
        if q == 2:
            return None, tiles, None
        up = pick(18 + 3 * q, jnp.concatenate([mine, theirs], axis=0))
        s_q[q + 1, 0] = joined(up)
        return up, tiles, send_skel(q + 1)

    def far_tiles(tiles):
        for tile in tiles:
            far_tile(*tile)

    def build_pair(e, k, flag):
        rows = pl.ds(pl.multiple_of(e * LEAF, LEAF), LEAF)
        cols = pl.ds(pl.multiple_of((e + k) * LEAF, LEAF), LEAF)
        mask = jnp.where(flag >= 0, 1.0, 0.0).astype(F32)
        high, low = split(jnp.exp(exponent(xhl[rows, :], n1[rows, :], xhl[cols, :], n2[cols, :])) * mask)
        tile_h[3 * e + k - 2] = high
        tile_l[3 * e + k - 2] = low

    def build(t):
        build_pair(t // 3 + 2, t % 3, neighbours[t // 3, 2 + t % 3])

    def near_target(j):
        total = None
        for o in (0, -1, -2):
            cols = pl.ds(pl.multiple_of((j + 2 + o) * LEAF, LEAF), LEAF)
            t = 3 * (j + o) - o
            part = times(vs[:, cols], tile_h[t + 4], tile_l[t + 4])
            total = part if total is None else total + part
        turned = None
        for o in (1, 2):
            cols = pl.ds(pl.multiple_of((j + 2 + o) * LEAF, LEAF), LEAF)
            t = 3 * j + o
            part = dot(tile_h[t + 4], vs[:, cols], 1, 1) + dot(tile_l[t + 4], vs[:, cols], 1, 1)
            turned = part if turned is None else turned + part
        turned = turned.T
        return total + (turned[:CLS] + turned[CLS:])

    def gram(pairs):
        sums = None
        for j in range(LV):
            stacks = {}

            def get(ref, at):
                if id(ref) not in stacks:
                    stacks[id(ref)] = stack(ref[:, pl.ds(at + j * LEAF, LEAF)])
                return stacks[id(ref)]

            parts = []
            for a, a0, b, b0 in pairs:
                bs = get(b, b0)
                parts.append(times(get(a, a0), bs[:CLS], bs[CLS:], 1))
            sums = parts if sums is None else [s + p for s, p in zip(sums, parts)]
        return sums

    class Sum:
        pass

    def sum_start(index, value):
        r = Sum()
        rows = value.shape[0]
        r.rows, r.index = pl.ds(0, rows), index
        ar_r0[index, 0, r.rows, :] = value
        r.copies = [send(ar_r0.at[index, 0, r.rows, :], ar_r0.at[index, 1, r.rows, :], partner)]
        return r

    def sum_step(r, stage):
        arrive(r.copies)
        if stage == 0:
            value = ar_r0[r.index, 0, r.rows, :] + ar_r0[r.index, 1, r.rows, :]
        else:
            at = r.index * 3 + stage - 1
            value = (ar_q[at, 0, r.rows, :] + ar_q[at, 1, r.rows, :]) + (
                ar_q[at, 2, r.rows, :] + ar_q[at, 3, r.rows, :]
            )
        if stage < 3:
            at = r.index * 3 + stage
            ar_q[at, 0, r.rows, :] = value
            r.copies = [
                send(ar_q.at[at, 0, r.rows, :], ar_q.at[at, s, r.rows, :], peer(stage, s)) for s in (1, 2, 3)
            ]
        return value

    def folded(m):
        return jnp.concatenate([m[:HALF], m[HALF:]], axis=1)

    def unfolded(m):
        return jnp.concatenate([m[:, :CLS], m[:, CLS:]], axis=0)

    def square_t(m):
        return jnp.concatenate([m, jnp.zeros_like(m)], axis=1)

    def low_pairs_t(m):
        return transposed(square_t(m))[:CLS, :CLS]

    def sym(m):
        return 0.5 * (m + transposed(square_t(m))[:CLS, :CLS])

    def inverse_of(m):
        row = lax.broadcasted_iota(I32, (CLS, CLS), 0)
        col = lax.broadcasted_iota(I32, (CLS, CLS), 1)
        return solve(m, jnp.where(row == col, 1.0, 0.0).astype(F32))[:, CLS:]

    loop2(2, 10, prepare)
    far_tiles([(i, *pair) for i, pair in enumerate(pairs)])
    loop(0, 2, build)
    own4, tiles3, copy_s = skel_core()
    load_b.wait()

    def split_b(e):
        split_columns(be, e)

    loop(2, 10, split_b)
    load_itp.wait()
    load_tra.wait()
    t0 = up_local(0)
    sum0 = sum_start(0, folded(gram([(be, OWN, be, OWN)])[0]))
    loop2(2, 6, build)
    up_core(0, t0)
    sum_step(sum0, 0)
    far_tiles(tiles3)
    loop2(6, 12, build)
    copy_s = forward_skel(0, copy_s)
    up_quad(0, t0, 0)
    sum_step(sum0, 1)
    own6, tiles4, copy_s = skel_quad(0, own4, copy_s)
    far_tiles(tiles4)
    loop2(12, 20, build)
    copy_s = forward_skel(1, copy_s)
    up_quad(0, t0, 1)
    sum_step(sum0, 2)
    own8, tiles6, copy_s = skel_quad(1, own6, copy_s)
    far_tiles(tiles6)

    def first_near(j):
        cols = pl.ds(pl.multiple_of((j + 2) * LEAF, LEAF), LEAF)
        ye[:, cols] = be[:, cols] + near_target(j)

    def at_halo(f):
        return lambda i: f(i + 8 * (i // 2))

    def at_edge(f):
        return lambda i: f(i + 4 * (i // 2))

    loop2(2, 6, first_near)
    copy_s = forward_skel(2, copy_s)
    up_quad(0, t0, 2)
    m0 = unfolded(sum_step(sum0, 3))
    _, tiles8, _ = skel_quad(2, own8, copy_s)
    halo_b = halo_columns(be)
    far_tiles(tiles8)
    down_top(0, t0)
    arrive(halo_x)

    def halo_setup(e):
        split_rows(e)
        prepare(e)

    loop(0, 4, at_halo(halo_setup))
    loop(20, 24, build)
    loop(0, 3, lambda i: build_pair((i + 1) // 2, 2 - i % 2, neighbours[i // 2, i % 2]))
    arrive(halo_b)
    loop(0, 4, at_halo(split_b))
    loop2(0, 4, at_edge(first_near))
    down_device(0, t0)

    def store_first(j, far):
        cols = pl.ds(OWN + j * LEAF, LEAF)
        ye[:, cols] = ye[:, cols] + far

    down_local(0, t0, store_first)

    def split_y(e):
        split_columns(ye, e)

    halo_y = halo_columns(ye)
    loop(2, 10, split_y)
    t1 = up_local(1)
    sum1 = sum_start(1, jnp.concatenate(gram([(be, OWN, ye, OWN), (ye, OWN, ye, OWN)]), axis=1))

    def second_near(j):
        cols = pl.ds(pl.multiple_of(j * LEAF, LEAF), LEAF)
        near[:, cols] = near_target(j)

    up_core(1, t1)
    sum_step(sum1, 0)
    low_pairs = tree_gram(t1)
    loop2(2, 4, second_near)
    up_quad(1, t1, 0)
    sum_step(sum1, 1)
    loop2(4, 6, second_near)
    inverse0 = inverse_of(sym(m0))
    up_quad(1, t1, 1)
    sum_step(sum1, 2)
    arrive(halo_y)
    loop(0, 4, at_halo(split_y))
    loop2(0, 4, at_edge(second_near))
    near_gram = gram([(ye, OWN, near, 0)])[0]
    up_quad(1, t1, 2)
    down_top(1, t1)
    moments = sum_step(sum1, 3)
    down_device(1, t1)
    bends = near_gram + low_pairs + low_pairs_t(low_pairs) + times_f32(w_r0[1, 0], t1.top, 1)
    curve = sum_start(2, folded(bends))

    def store_second(j, far):
        cols = pl.ds(j * LEAF, LEAF)
        near[:, cols] = near[:, cols] + far + ye[:, pl.ds(OWN + j * LEAF, LEAF)]

    m0 = sym(m0)
    m1 = moments[:, :CLS]
    m2 = moments[:, CLS:]
    sum_step(curve, 0)
    step = solve(sym(m1), m0)
    alpha = step[:, CLS:]
    alpha_t = transposed(step)[CLS:, :CLS]
    cross = times_f32(m1, alpha)
    new = m0 - 2.0 * sym(cross) + sym(times_f32(times_f32(alpha_t, m2), alpha))
    beta = times_f32(inverse0, new)
    beta_t = low_pairs_t(beta)
    row = lax.broadcasted_iota(I32, (CLS, CLS), 0)
    col = lax.broadcasted_iota(I32, (CLS, CLS), 1)
    unit = jnp.where(row == col, 1.0, 0.0)
    plus = unit + beta
    plus_t = unit + beta_t
    sum_step(curve, 1)
    down_local(1, t1, store_second)
    sum_step(curve, 2)

    alpha_s = stack(alpha_t)
    plus_s = stack(plus_t)

    def mix(matrix_s, x):
        high, low = split(x)
        return times(matrix_s, high, low)

    for copy in halo_b + halo_y:
        copy.wait_send()

    def update(j):
        cols = pl.ds(pl.multiple_of(j * 2 * LEAF, LEAF), 2 * LEAF)
        wide = pl.ds(pl.multiple_of((j + 1) * 2 * LEAF, LEAF), 2 * LEAF)
        old, image = be[:, wide], ye[:, wide]
        start = mix(alpha_s, image)
        high, low = split(mix(plus_s, old) - start)
        vs[pl.ds(0, CLS), wide] = high
        vs[pl.ds(CLS, CLS), wide] = low
        near[:, cols] = mix(plus_s, image) - mix(alpha_s, near[:, cols])
        be[:, wide] = mix(alpha_s, old)
        ye[:, wide] = old - start

    loop(0, LV // 2, update)
    outs = [
        load(be.at[:, own_rows], x_out), load(ye.at[:, own_rows], r_out),
        load(vs.at[:, own_rows], d_out), load(near, a_out),
    ]
    known = times_f32(times_f32(plus_t, m1), plus) - 2.0 * sym(times_f32(times_f32(plus_t, m2), alpha))
    known = known + times_f32(times_f32(alpha_t, m2), alpha)
    bends = unfolded(sum_step(curve, 3))
    curvature = sym(known + times_f32(times_f32(alpha_t, bends), alpha))
    coef[...] = transposed(solve(curvature, new))[CLS:, :]
    outs.append(load(coef, c_out))
    for copy in outs:
        copy.wait()
    for copy in sent:
        if not any(copy is done for done in halo_b + halo_y):
            copy.wait_send()


def finish(coef, x0, r1, direction, image, x_out, r_out, cv, xv, rv, dv, av, in_sem, out_sem):
    count = LV // 2
    refs = ((direction, dv), (image, av), (x0, xv), (r1, rv))
    chunks = [pl.ds(j * 2 * LEAF, 2 * LEAF) for j in range(count)]
    loads = [pltpu.make_async_copy(coef, cv, in_sem.at[4 * count])]
    for j in range(count):
        for i, (src, dst) in enumerate(refs):
            loads.append(
                pltpu.make_async_copy(src.at[:, chunks[j]], dst.at[:, chunks[j]], in_sem.at[4 * j + i])
            )
    for copy in loads:
        copy.start()
    loads[0].wait()
    last_s = stack(cv[:, :CLS])
    stores = []
    for j in range(count):
        for copy in loads[4 * j + 1 : 4 * j + 5]:
            copy.wait()
        part = chunks[j]
        xv[:, part] = xv[:, part] + times(last_s, dv[:CLS, part], dv[CLS:, part])
        high, low = split(av[:, part])
        rv[:, part] = rv[:, part] - times(last_s, high, low)
        for i, (src, dst) in enumerate(((xv, x_out), (rv, r_out))):
            copy = pltpu.make_async_copy(src.at[:, part], dst.at[:, part], out_sem.at[2 * j + i])
            copy.start()
            stores.append(copy)
    for copy in stores:
        copy.wait()


def solution(mesh):
    any_space = pl.BlockSpec(memory_space=pl.ANY)
    vmem = pltpu.VMEM

    def device(points, right_side, neighbours, leaf_interp, leaf_skeleton, node_skeleton, node_gain, transfer):
        out = jax.ShapeDtypeStruct(right_side.shape, F32)
        both = jax.ShapeDtypeStruct((2 * CLS, LV * LEAF), BF16)
        x0, r1, direction, image, coef = pl.pallas_call(
            body,
            out_shape=(out, out, both, out, jax.ShapeDtypeStruct((CLS, 128), F32)),
            in_specs=[
                any_space, any_space, pl.BlockSpec(memory_space=pltpu.SMEM), any_space,
                any_space, any_space, any_space, any_space,
            ],
            out_specs=(any_space,) * 5,
            scratch_shapes=[
                vmem((WIDE, DIM), F32),
                vmem((WIDE, 2 * DIM), BF16),
                vmem((WIDE, DIM), BF16),
                vmem((WIDE, DIM), BF16),
                vmem((28, LEAF, LEAF), BF16),
                vmem((28, LEAF, LEAF), BF16),
                vmem((CLS, WIDE), F32),
                vmem((CLS, WIDE), F32),
                vmem((CLS, LV * LEAF), F32),
                vmem((2 * CLS, WIDE), BF16),
                vmem((LV, LEAF, SKEL), F32),
                vmem((9, 2, SKEL, SKEL), F32),
                vmem((9, 8, SKEL), F32),
                vmem((9, 8, SKEL), I32),
                vmem((LV, SKEL), I32),
                vmem((128, SKEL), F32),
                vmem((SKEL, 128), I32),
                vmem((14, SKEL, SKEL), BF16),
                vmem((14, SKEL, SKEL), BF16),
                vmem((2, SKEL, DIM), F32),
                vmem((3, 4, SKEL, DIM), F32),
                vmem((2, 2, CLS, SKEL), F32),
                vmem((6, 4, HALF, SKEL), F32),
                vmem((2, CLS, SKEL), F32),
                vmem((3, 2, CLS, 128), F32),
                vmem((9, 4, CLS, 128), F32),
                vmem((CLS, 128), F32),
                pltpu.SemaphoreType.DMA((28,)),
                pltpu.SemaphoreType.DMA((72,)),
                pltpu.SemaphoreType.DMA((72,)),
            ],
            compiler_params=pltpu.CompilerParams(
                collective_id=0, has_side_effects=True, vmem_limit_bytes=67043328
            ),
        )(points, right_side, neighbours, leaf_interp, leaf_skeleton, node_skeleton, node_gain, transfer)
        return pl.pallas_call(
            finish,
            out_shape=(out, out),
            in_specs=[any_space] * 5,
            out_specs=(any_space, any_space),
            scratch_shapes=[vmem((CLS, 128), F32)]
            + [vmem((CLS, LV * LEAF), F32)] * 2
            + [vmem((2 * CLS, LV * LEAF), BF16), vmem((CLS, LV * LEAF), F32)]
            + [pltpu.SemaphoreType.DMA((2 * LV + 1,)), pltpu.SemaphoreType.DMA((LV,))],
        )(coef, x0, r1, direction, image)

    in_specs = (
        P("leaf", None), P(None, "leaf"), P("leaf", None), P("leaf", None, None),
        P("leaf", None), P(), P(), P(),
    )
    out_specs = (P(None, "leaf"), P(None, "leaf"))
    return jax.shard_map(device, mesh=mesh, in_specs=in_specs, out_specs=out_specs, check_vma=False)
```

```python
import functools

import jax
import jax.numpy as jnp
from jax import lax
from jax.experimental import pallas as pl
from jax.experimental.pallas import tpu as pltpu
from jax.sharding import PartitionSpec as P

MESH = pl.DeviceIdType.MESH
F32 = jnp.float32
BF16 = jnp.bfloat16
I32 = jnp.int32

LEAF, SKEL, DIM, CLS = 512, 256, 128, 64
LV = 8
LEAVES = 1024
HALF = CLS // 2
OWN = 2 * LEAF
WIDE = (LV + 4) * LEAF


def split(x):
    high = x.astype(BF16)
    return high, (x - high.astype(F32)).astype(BF16)


def dot(a, b, ca=1, cb=0):
    return lax.dot_general(a, b, (((ca,), (cb,)), ((), ())), preferred_element_type=F32)


def times(stacked, high, low, cb=0):
    rows = stacked.shape[0] // 2
    both = dot(stacked, high, 1, cb)
    return both[:rows] + both[rows:] + dot(stacked[:rows], low, 1, cb)


def stack(x):
    return jnp.concatenate(split(x), axis=0)


def times_f32(a, b, cb=0):
    high, low = split(b)
    return times(stack(a), high, low, cb)


def norm_columns(x):
    half = -0.5 * jnp.sum(x * x, axis=1, keepdims=True)
    half = jnp.broadcast_to(half, x.shape)
    first = half.astype(BF16).astype(F32)
    rest = half - first
    second = rest.astype(BF16).astype(F32)
    third = rest - second
    lane = lax.broadcasted_iota(I32, x.shape, 1)
    parts = jnp.where(lane % 3 == 0, first, jnp.where(lane % 3 == 1, second, third))
    ones = jnp.ones_like(parts)
    zero = jnp.zeros_like(parts)
    low = jnp.where(lane < 3, ones, jnp.where(lane < 6, parts, zero))
    high = jnp.where(lane < 3, parts, jnp.where(lane < 6, ones, zero))
    return low.astype(BF16), high.astype(BF16)


def exponent(a_hl, a_n1, b_hl, b_n2):
    a_h = a_hl[:, :DIM]
    b_h, b_l = b_hl[:, :DIM], b_hl[:, DIM:]
    first = dot(a_hl, jnp.concatenate([b_h, b_h], axis=1), 1, 1)
    second = dot(
        jnp.concatenate([a_h, a_n1], axis=1), jnp.concatenate([b_l, b_n2], axis=1), 1, 1
    )
    return first + second


def transposed(top):
    return jnp.concatenate([top, jnp.zeros_like(top)], axis=0).T


def solve(matrix, target):
    work = jnp.concatenate([matrix, target], axis=1)
    row_id = lax.broadcasted_iota(I32, work.shape, 0)
    block = 4
    for start in range(0, CLS, block):
        columns = [
            jnp.broadcast_to(work[:, start + i : start + i + 1], work.shape) for i in range(block)
        ]
        for i in range(block):
            k = start + i
            here = row_id == k
            inverse = 1.0 / columns[i][k : k + 1, :]
            pivot = work[k : k + 1, :] * inverse
            work = jnp.where(here, pivot, work - columns[i] * pivot)
            for j in range(i + 1, block):
                entry = columns[j][k : k + 1, :] * inverse
                columns[j] = jnp.where(here, entry, columns[j] - columns[i] * entry)
    return work


def body(
    points, right_side, neighbours, leaf_interp, leaf_skeleton, node_skeleton, node_gain, transfer,
    x_out, r_out, d_out, a_out, c_out,
    xe, xhl, n1, n2, tile_h, tile_l, be, ye, near, vs, itp, tra, gw, nw, lsk, idx_rows, idx_cols,
    fh, fl, s_r0, s_q, w_r0, w_q, u4, ar_r0, ar_q, coef,
    local_sem, send_sem, recv_sem,
):
    me = lax.axis_index("leaf")
    core = me % 2
    chip = me // 2
    left = (me + 127) % 128
    right = (me + 1) % 128
    partner = me + 1 - 2 * core

    def peer(axis, s):
        stride = (2, 8, 32)[axis]
        at = (me // stride) % 4
        if s == 1:
            other = at + 1 - 2 * (at % 2)
        elif s == 2:
            other = at + 2 - 4 * (at // 2)
        else:
            other = 3 - at
        return me + (other - at) * stride

    def xor(n, s):
        if s == 1:
            return n + 1 - 2 * (n % 2)
        if s == 2:
            return n + 2 - 4 * ((n // 2) % 2)
        return xor(xor(n, 1), 2)

    loads = []

    def load(src, dst):
        copy = pltpu.make_async_copy(src, dst, local_sem.at[len(loads)])
        copy.start()
        loads.append(copy)
        return copy

    own_rows = pl.ds(OWN, LV * LEAF)
    load_points = load(points, xe.at[own_rows, :])
    load_small = [load(leaf_skeleton, lsk)]

    def gain_row(level):
        return 2 * LEAVES - 2 * (LEAVES >> level)

    def skel_row(level):
        return LEAVES - 2 * (LEAVES >> level)

    gain_node = [me * 8, me * 4, me * 2, me, me // 2, me // 4, me // 8, me // 16, me // 32]
    for level in range(9):
        if level < 8:
            at = pl.multiple_of(gain_row(level) + (gain_node[level] // 8) * 8, 8)
            load_small.append(load(node_gain.at[pl.ds(at, 8), :], gw.at[level]))
        else:
            load_small.append(load(node_gain.at[pl.ds(2040, 6), :], gw.at[level, pl.ds(0, 6), :]))
    skel_node = [None, me * 4, me * 2, me, me // 2, me // 4, me // 8, me // 16]
    for level in range(1, 9):
        if level < 8:
            at = pl.multiple_of(skel_row(level) + (skel_node[level] // 8) * 8, 8)
            load_small.append(load(node_skeleton.at[pl.ds(at, 8), :], nw.at[level]))
        else:
            load_small.append(load(node_skeleton.at[pl.ds(1016, 6), :], nw.at[level, pl.ds(0, 6), :]))
    load_b = load(right_side, be.at[:, own_rows])
    load_itp = load(leaf_interp, itp)
    load_tra = load(transfer, tra)

    peers = [partner, left, right] + [peer(a, s) for a in range(3) for s in (1, 2, 3)]
    barrier = pltpu.get_barrier_semaphore()
    for other in peers:
        pl.semaphore_signal(barrier, inc=1, device_id=(other,), device_id_type=MESH)

    sent = []

    def send(src, dst, device):
        k = len(sent)
        copy = pltpu.make_async_remote_copy(
            src_ref=src, dst_ref=dst, send_sem=send_sem.at[k], recv_sem=recv_sem.at[k],
            device_id=(device,), device_id_type=MESH,
        )
        copy.start()
        sent.append(copy)
        return copy

    def send_quad(buf, index, axis):
        return [send(buf.at[index, 0], buf.at[index, s], peer(axis, s)) for s in (1, 2, 3)]

    def arrive(copies):
        for copy in copies:
            copy.wait_recv()

    first, last = pl.ds(OWN, OWN), pl.ds(OWN + (LV - 2) * LEAF, OWN)
    head, tail = pl.ds(0, OWN), pl.ds(OWN + LV * LEAF, OWN)

    def halo_rows(ref):
        return [send(ref.at[first, :], ref.at[tail, :], left), send(ref.at[last, :], ref.at[head, :], right)]

    def halo_columns(ref):
        return [send(ref.at[:, first], ref.at[:, tail], left), send(ref.at[:, last], ref.at[:, head], right)]

    def split_rows(e):
        rows = pl.ds(pl.multiple_of(e * LEAF, LEAF), LEAF)
        xhl[rows, :] = jnp.concatenate(split(xe[rows, :]), axis=1)

    def prepare(e):
        rows = pl.ds(pl.multiple_of(e * LEAF, LEAF), LEAF)
        a, b = norm_columns(xe[rows, :])
        n1[rows, :] = a
        n2[rows, :] = b

    def split_columns(src, e):
        cols = pl.ds(pl.multiple_of(e * LEAF, LEAF), LEAF)
        high, low = split(src[:, cols])
        vs[pl.ds(0, CLS), cols] = high
        vs[pl.ds(CLS, CLS), cols] = low

    def loop(start, stop, f):
        def step(i, carry):
            f(i)
            return carry

        lax.fori_loop(start, stop, step, 0)

    load_points.wait()
    pl.semaphore_wait(barrier, len(peers))
    halo_x = halo_rows(xe)
    loop(2, 10, split_rows)

    def loop2(start, stop, f):
        def step(i, carry):
            f(start + 2 * i)
            f(start + 2 * i + 1)
            return carry

        lax.fori_loop(0, (stop - start) // 2, step, 0)

    for copy in load_small:
        copy.wait()
    idx_rows[...] = jnp.zeros_like(idx_rows)
    idx_rows[pl.ds(0, 8), :] = lsk[...].astype(F32)

    def put_index(slot, level, row, parity):
        index = nw[level, pl.ds(row, 1), :] + 256 * parity
        index = jnp.where(index >= 512, index - 512, index)
        idx_rows[pl.ds(slot, 1), :] = index.astype(F32)

    for i in range(4):
        put_index(8 + i, 1, (me * 4) % 8 + i, 0)
    for i in range(2):
        put_index(12 + i, 2, (me * 2) % 8 + i, 0)
    put_index(14, 3, me % 8, 0)
    put_index(15, 4, (me // 2) % 8, me % 2)
    n4, n6, n8 = me // 2, me // 8, me // 32
    quad_level = (4, 6, 8)
    quad_node = (n4, n6, n8)
    for q in range(3):
        level, node = quad_level[q], quad_node[q]
        parent = node // 2
        lv = min(level + 1, 8)
        base = 4 if level == 8 else 0
        put_index(16 + 3 * q, lv, base + parent % 8, node % 2)
        put_index(17 + 3 * q, lv, base + xor(parent, 1) % 8, node % 2)
        if q < 2:
            grand = parent // 2
            put_index(18 + 3 * q, level + 2, grand % 8, parent % 2)
    idx_cols[...] = idx_rows[...].T.astype(I32)

    def pick(slot, rows_hl):
        lane = lax.broadcasted_iota(I32, (SKEL, 2 * SKEL), 1)
        chosen = jnp.broadcast_to(idx_cols[:, slot : slot + 1], (SKEL, 2 * SKEL))
        one_hot = jnp.where(lane == chosen, 1.0, 0.0).astype(BF16)
        return dot(one_hot, rows_hl).astype(BF16)

    def joined(hl):
        return hl[:, :DIM].astype(F32) + hl[:, DIM:].astype(F32)

    def far_tile(slot, sibling_hl, own_hl):
        a1, _ = norm_columns(joined(sibling_hl))
        _, b2 = norm_columns(joined(own_hl))
        high, low = split(jnp.exp(exponent(sibling_hl, a1, own_hl, b2)))
        fh[slot] = high
        fl[slot] = low

    skel = [pick(j, xhl[pl.ds(OWN + j * LEAF, LEAF), :]) for j in range(LV)]
    index = 8
    pairs = []
    while len(skel) > 1:
        parents = []
        for i in range(len(skel) // 2):
            pairs.append((skel[2 * i + 1], skel[2 * i]))
            parents.append(pick(index, jnp.concatenate(skel[2 * i : 2 * i + 2], axis=0)))
            index += 1
        skel = parents
    skel3 = skel[0]
    s_r0[0] = joined(skel3)
    copy_s = [send(s_r0.at[0], s_r0.at[1], partner)]

    def gain(level, node):
        row = node % 8
        return gw[level, pl.ds(row, 1), :]

    class Tree:
        pass

    def up_local(it):
        t = Tree()
        t.levels = []
        rows = []
        for j in range(LV):
            v = vs[:, pl.ds(OWN + j * LEAF, LEAF)]
            high, low = split(itp[j])
            rows.append(times(v, high, low))
        for level in range(3):
            t.levels.append(rows)
            count = len(rows)
            lefts = jnp.concatenate(
                [rows[n] * gain(level, me * count + n) for n in range(0, count, 2)], axis=0
            )
            rights = jnp.concatenate(
                [rows[n] * gain(level, me * count + n) for n in range(1, count, 2)], axis=0
            )
            joint = times_f32(lefts, tra[level, 0]) + times_f32(rights, tra[level, 1])
            rows = [joint[n * CLS : (n + 1) * CLS] for n in range(count // 2)]
        w_r0[it, 0] = rows[0]
        t.copies = [send(w_r0.at[it, 0], w_r0.at[it, 1], partner)]
        return t

    my_half = pl.ds(pl.multiple_of(core * HALF, HALF), HALF)

    def up_core(it, t):
        arrive(t.copies)
        own = w_r0[it, 0, my_half, :] * gain(3, me)
        sib = w_r0[it, 1, my_half, :] * gain(3, partner)
        w_q[it * 3, 0] = times_f32(own, tra[3, core]) + times_f32(sib, tra[3, 1 - core])
        t.copies = send_quad(w_q, it * 3, 0)
        t.sib = {}

    def up_quad(it, t, q):
        arrive(t.copies)
        level, node = quad_level[q], quad_node[q]
        parity = node % 2
        four = [w_q[it * 3 + q, s] for s in range(4)]
        t.sib[level] = four[1]
        if q == 2:
            a = four[2] * gain(level, xor(node, 2))
            b = four[3] * gain(level, xor(node, 3))
            t.sib[level + 1] = times_f32(a, tra[level, parity]) + times_f32(b, tra[level, 1 - parity])
            return
        a = jnp.concatenate([four[0] * gain(level, node), four[2] * gain(level, xor(node, 2))], axis=0)
        b = jnp.concatenate(
            [four[1] * gain(level, xor(node, 1)), four[3] * gain(level, xor(node, 3))], axis=0
        )
        two = times_f32(a, tra[level, parity]) + times_f32(b, tra[level, 1 - parity])
        t.sib[level + 1] = two[HALF:]
        parent = node // 2
        parity = parent % 2
        a = two[:HALF] * gain(level + 1, parent)
        b = two[HALF:] * gain(level + 1, xor(parent, 1))
        w_q[it * 3 + q + 1, 0] = times_f32(a, tra[level + 1, parity]) + times_f32(
            b, tra[level + 1, 1 - parity]
        )
        t.copies = send_quad(w_q, it * 3 + q + 1, q + 1)

    def down_top(it, t):
        pot = times(stack(t.sib[9]), fh[13], fl[13])
        for level in range(8, 3, -1):
            node = me // (1 << (level - 3))
            pot = times_f32(pot, tra[level, node % 2], 1) * gain(level, node)
            pot = pot + times(stack(t.sib[level]), fh[level + 4], fl[level + 4])
        u4[it, my_half, :] = pot
        t.copies = [send(u4.at[it, my_half, :], u4.at[it, my_half, :], partner)]

    def down_device(it, t):
        arrive(t.copies)
        pot = times_f32(u4[it], tra[3, core], 1) * gain(3, me)
        t.top = pot + times(stack(w_r0[it, 1]), fh[7], fl[7])

    def tree_gram(t):
        total = None
        slot = 0
        for level in range(3):
            rows = t.levels[level]
            for i in range(len(rows) // 2):
                part = times(stack(rows[2 * i + 1]), fh[slot], fl[slot])
                part = times_f32(rows[2 * i], part, 1)
                total = part if total is None else total + part
                slot += 1
        return total

    def down_local(it, t, store):
        pot = t.top
        slot = 7
        for level in (2, 1, 0):
            rows = t.levels[level]
            count = len(rows)
            slot -= count // 2
            stacked = stack(pot)
            out = []
            lefts = times(stacked, *split(tra[level, 0]), 1)
            rights = times(stacked, *split(tra[level, 1]), 1)
            for n in range(count):
                part = (lefts, rights)[n % 2][(n // 2) * CLS : (n // 2 + 1) * CLS]
                part = part * gain(level, me * count + n)
                other = stack(rows[n + 1 - 2 * (n % 2)])
                f = slot + n // 2
                out.append(part + times(other, fh[f], fl[f], n % 2))
            pot = jnp.concatenate(out, axis=0)
        for j in range(LV):
            high, low = split(itp[j])
            store(j, times(stack(pot[j * CLS : (j + 1) * CLS]), high, low, 1))

    my_points = pl.ds(pl.multiple_of(core * 128, 128), 128)

    def send_skel(q):
        return [
            send(s_q.at[q, 0, my_points, :], s_q.at[q, s, my_points, :], peer(q, s)) for s in (1, 2, 3)
        ]

    def forward_skel(q, copies):
        arrive(copies)
        part = s_q.at[q, pl.ds(1, 3), my_points, :]
        return [send(part, part, partner)]

    def skel_core():
        arrive(copy_s)
        other = jnp.concatenate(split(s_r0[1]), axis=1)
        own = pick(15, jnp.concatenate([skel3, other], axis=0))
        s_q[0, 0] = joined(own)
        return (own, [(7, other, skel3)], send_skel(0))

    def skel_quad(q, own, copies):
        arrive(copies)
        s1, s2, s3 = [jnp.concatenate(split(s_q[q, s]), axis=1) for s in (1, 2, 3)]
        mine = pick(16 + 3 * q, jnp.concatenate([own, s1], axis=0))
        theirs = pick(17 + 3 * q, jnp.concatenate([s2, s3], axis=0))
        tiles = [(8 + 2 * q, s1, own), (9 + 2 * q, theirs, mine)]
        if q == 2:
            return None, tiles, None
        up = pick(18 + 3 * q, jnp.concatenate([mine, theirs], axis=0))
        s_q[q + 1, 0] = joined(up)
        return up, tiles, send_skel(q + 1)

    def far_tiles(tiles):
        for tile in tiles:
            far_tile(*tile)

    def build_pair(e, k, flag):
        rows = pl.ds(pl.multiple_of(e * LEAF, LEAF), LEAF)
        cols = pl.ds(pl.multiple_of((e + k) * LEAF, LEAF), LEAF)
        mask = jnp.where(flag >= 0, 1.0, 0.0).astype(F32)
        high, low = split(jnp.exp(exponent(xhl[rows, :], n1[rows, :], xhl[cols, :], n2[cols, :])) * mask)
        tile_h[3 * e + k - 2] = high
        tile_l[3 * e + k - 2] = low

    def build(t):
        build_pair(t // 3 + 2, t % 3, neighbours[t // 3, 2 + t % 3])

    def near_target(j):
        total = None
        for o in (0, -1, -2):
            cols = pl.ds(pl.multiple_of((j + 2 + o) * LEAF, LEAF), LEAF)
            t = 3 * (j + o) - o
            part = times(vs[:, cols], tile_h[t + 4], tile_l[t + 4])
            total = part if total is None else total + part
        turned = None
        for o in (1, 2):
            cols = pl.ds(pl.multiple_of((j + 2 + o) * LEAF, LEAF), LEAF)
            t = 3 * j + o
            part = dot(tile_h[t + 4], vs[:, cols], 1, 1) + dot(tile_l[t + 4], vs[:, cols], 1, 1)
            turned = part if turned is None else turned + part
        turned = turned.T
        return total + (turned[:CLS] + turned[CLS:])

    def gram(pairs):
        sums = None
        for j in range(LV):
            stacks = {}

            def get(ref, at):
                if id(ref) not in stacks:
                    stacks[id(ref)] = stack(ref[:, pl.ds(at + j * LEAF, LEAF)])
                return stacks[id(ref)]

            parts = []
            for a, a0, b, b0 in pairs:
                bs = get(b, b0)
                parts.append(times(get(a, a0), bs[:CLS], bs[CLS:], 1))
            sums = parts if sums is None else [s + p for s, p in zip(sums, parts)]
        return sums

    class Sum:
        pass

    def sum_start(index, value):
        r = Sum()
        rows = value.shape[0]
        r.rows, r.index = pl.ds(0, rows), index
        ar_r0[index, 0, r.rows, :] = value
        r.copies = [send(ar_r0.at[index, 0, r.rows, :], ar_r0.at[index, 1, r.rows, :], partner)]
        return r

    def sum_step(r, stage):
        arrive(r.copies)
        if stage == 0:
            value = ar_r0[r.index, 0, r.rows, :] + ar_r0[r.index, 1, r.rows, :]
        else:
            at = r.index * 3 + stage - 1
            value = (ar_q[at, 0, r.rows, :] + ar_q[at, 1, r.rows, :]) + (
                ar_q[at, 2, r.rows, :] + ar_q[at, 3, r.rows, :]
            )
        if stage < 3:
            at = r.index * 3 + stage
            ar_q[at, 0, r.rows, :] = value
            r.copies = [
                send(ar_q.at[at, 0, r.rows, :], ar_q.at[at, s, r.rows, :], peer(stage, s)) for s in (1, 2, 3)
            ]
        return value

    def folded(m):
        return jnp.concatenate([m[:HALF], m[HALF:]], axis=1)

    def unfolded(m):
        return jnp.concatenate([m[:, :CLS], m[:, CLS:]], axis=0)

    def square_t(m):
        return jnp.concatenate([m, jnp.zeros_like(m)], axis=1)

    def low_pairs_t(m):
        return transposed(square_t(m))[:CLS, :CLS]

    def sym(m):
        return 0.5 * (m + transposed(square_t(m))[:CLS, :CLS])

    def inverse_of(m):
        row = lax.broadcasted_iota(I32, (CLS, CLS), 0)
        col = lax.broadcasted_iota(I32, (CLS, CLS), 1)
        return solve(m, jnp.where(row == col, 1.0, 0.0).astype(F32))[:, CLS:]

    loop2(2, 10, prepare)
    own4, tiles3, copy_s = skel_core()
    far_tiles([(i, *pair) for i, pair in enumerate(pairs)])
    loop(0, 2, build)
    load_b.wait()

    def split_b(e):
        split_columns(be, e)

    loop(2, 10, split_b)
    load_itp.wait()
    load_tra.wait()
    t0 = up_local(0)
    sum0 = sum_start(0, folded(gram([(be, OWN, be, OWN)])[0]))
    loop2(2, 6, build)
    up_core(0, t0)
    sum_step(sum0, 0)
    far_tiles(tiles3)
    loop2(6, 12, build)
    copy_s = forward_skel(0, copy_s)
    up_quad(0, t0, 0)
    sum_step(sum0, 1)
    own6, tiles4, copy_s = skel_quad(0, own4, copy_s)
    far_tiles(tiles4)
    loop2(12, 20, build)
    copy_s = forward_skel(1, copy_s)
    up_quad(0, t0, 1)
    sum_step(sum0, 2)
    own8, tiles6, copy_s = skel_quad(1, own6, copy_s)
    far_tiles(tiles6)

    def first_near(j):
        cols = pl.ds(pl.multiple_of((j + 2) * LEAF, LEAF), LEAF)
        ye[:, cols] = be[:, cols] + near_target(j)

    def at_halo(f):
        return lambda i: f(i + 8 * (i // 2))

    def at_edge(f):
        return lambda i: f(i + 4 * (i // 2))

    loop2(2, 6, first_near)
    copy_s = forward_skel(2, copy_s)
    up_quad(0, t0, 2)
    m0 = unfolded(sum_step(sum0, 3))
    _, tiles8, _ = skel_quad(2, own8, copy_s)
    halo_b = halo_columns(be)
    far_tiles(tiles8)
    down_top(0, t0)
    arrive(halo_x)

    def halo_setup(e):
        split_rows(e)
        prepare(e)

    loop(0, 4, at_halo(halo_setup))
    loop(20, 24, build)
    loop(0, 3, lambda i: build_pair((i + 1) // 2, 2 - i % 2, neighbours[i // 2, i % 2]))
    arrive(halo_b)
    loop(0, 4, at_halo(split_b))
    loop2(0, 4, at_edge(first_near))
    down_device(0, t0)

    def store_first(j, far):
        cols = pl.ds(OWN + j * LEAF, LEAF)
        ye[:, cols] = ye[:, cols] + far

    down_local(0, t0, store_first)

    def split_y(e):
        split_columns(ye, e)

    halo_y = halo_columns(ye)
    loop(2, 10, split_y)
    t1 = up_local(1)
    sum1 = sum_start(1, jnp.concatenate(gram([(be, OWN, ye, OWN), (ye, OWN, ye, OWN)]), axis=1))

    def second_near(j):
        cols = pl.ds(pl.multiple_of(j * LEAF, LEAF), LEAF)
        near[:, cols] = near_target(j)

    up_core(1, t1)
    sum_step(sum1, 0)
    low_pairs = tree_gram(t1)
    loop2(2, 4, second_near)
    up_quad(1, t1, 0)
    sum_step(sum1, 1)
    loop2(4, 6, second_near)
    inverse0 = inverse_of(sym(m0))
    up_quad(1, t1, 1)
    sum_step(sum1, 2)
    arrive(halo_y)
    loop(0, 4, at_halo(split_y))
    loop2(0, 4, at_edge(second_near))
    near_gram = gram([(ye, OWN, near, 0)])[0]
    up_quad(1, t1, 2)
    down_top(1, t1)
    moments = sum_step(sum1, 3)
    down_device(1, t1)
    bends = near_gram + low_pairs + low_pairs_t(low_pairs) + times_f32(w_r0[1, 0], t1.top, 1)
    curve = sum_start(2, folded(bends))

    def store_second(j, far):
        cols = pl.ds(j * LEAF, LEAF)
        near[:, cols] = near[:, cols] + far + ye[:, pl.ds(OWN + j * LEAF, LEAF)]

    m0 = sym(m0)
    m1 = moments[:, :CLS]
    m2 = moments[:, CLS:]
    sum_step(curve, 0)
    step = solve(sym(m1), m0)
    alpha = step[:, CLS:]
    alpha_t = transposed(step)[CLS:, :CLS]
    cross = times_f32(m1, alpha)
    new = m0 - 2.0 * sym(cross) + sym(times_f32(times_f32(alpha_t, m2), alpha))
    beta = times_f32(inverse0, new)
    beta_t = low_pairs_t(beta)
    row = lax.broadcasted_iota(I32, (CLS, CLS), 0)
    col = lax.broadcasted_iota(I32, (CLS, CLS), 1)
    unit = jnp.where(row == col, 1.0, 0.0)
    plus = unit + beta
    plus_t = unit + beta_t
    sum_step(curve, 1)
    down_local(1, t1, store_second)
    sum_step(curve, 2)

    alpha_s = stack(alpha_t)
    plus_s = stack(plus_t)

    def mix(matrix_s, x):
        high, low = split(x)
        return times(matrix_s, high, low)

    for copy in halo_b + halo_y:
        copy.wait_send()

    def update(j):
        cols = pl.ds(pl.multiple_of(j * 2 * LEAF, LEAF), 2 * LEAF)
        wide = pl.ds(pl.multiple_of((j + 1) * 2 * LEAF, LEAF), 2 * LEAF)
        old, image = be[:, wide], ye[:, wide]
        start = mix(alpha_s, image)
        high, low = split(mix(plus_s, old) - start)
        vs[pl.ds(0, CLS), wide] = high
        vs[pl.ds(CLS, CLS), wide] = low
        near[:, cols] = mix(plus_s, image) - mix(alpha_s, near[:, cols])
        be[:, wide] = mix(alpha_s, old)
        ye[:, wide] = old - start

    loop(0, LV // 2, update)
    outs = [
        load(be.at[:, own_rows], x_out), load(ye.at[:, own_rows], r_out),
        load(vs.at[:, own_rows], d_out), load(near, a_out),
    ]
    known = times_f32(times_f32(plus_t, m1), plus) - 2.0 * sym(times_f32(times_f32(plus_t, m2), alpha))
    known = known + times_f32(times_f32(alpha_t, m2), alpha)
    bends = unfolded(sum_step(curve, 3))
    curvature = sym(known + times_f32(times_f32(alpha_t, bends), alpha))
    coef[...] = transposed(solve(curvature, new))[CLS:, :]
    outs.append(load(coef, c_out))
    for copy in outs:
        copy.wait()
    for copy in sent:
        if not any(copy is done for done in halo_b + halo_y):
            copy.wait_send()


def finish(coef, x0, r1, direction, image, x_out, r_out, cv, xv, rv, dv, av, in_sem, out_sem):
    count = LV // 2
    refs = ((direction, dv), (image, av), (x0, xv), (r1, rv))
    chunks = [pl.ds(j * 2 * LEAF, 2 * LEAF) for j in range(count)]
    loads = [pltpu.make_async_copy(coef, cv, in_sem.at[4 * count])]
    for j in range(count):
        for i, (src, dst) in enumerate(refs):
            loads.append(
                pltpu.make_async_copy(src.at[:, chunks[j]], dst.at[:, chunks[j]], in_sem.at[4 * j + i])
            )
    for copy in loads:
        copy.start()
    loads[0].wait()
    last_s = stack(cv[:, :CLS])
    stores = []
    for j in range(count):
        for copy in loads[4 * j + 1 : 4 * j + 5]:
            copy.wait()
        part = chunks[j]
        xv[:, part] = xv[:, part] + times(last_s, dv[:CLS, part], dv[CLS:, part])
        high, low = split(av[:, part])
        rv[:, part] = rv[:, part] - times(last_s, high, low)
        for i, (src, dst) in enumerate(((xv, x_out), (rv, r_out))):
            copy = pltpu.make_async_copy(src.at[:, part], dst.at[:, part], out_sem.at[2 * j + i])
            copy.start()
            stores.append(copy)
    for copy in stores:
        copy.wait()


def solution(mesh):
    any_space = pl.BlockSpec(memory_space=pl.ANY)
    vmem = pltpu.VMEM

    def device(points, right_side, neighbours, leaf_interp, leaf_skeleton, node_skeleton, node_gain, transfer):
        out = jax.ShapeDtypeStruct(right_side.shape, F32)
        both = jax.ShapeDtypeStruct((2 * CLS, LV * LEAF), BF16)
        x0, r1, direction, image, coef = pl.pallas_call(
            body,
            out_shape=(out, out, both, out, jax.ShapeDtypeStruct((CLS, 128), F32)),
            in_specs=[
                any_space, any_space, pl.BlockSpec(memory_space=pltpu.SMEM), any_space,
                any_space, any_space, any_space, any_space,
            ],
            out_specs=(any_space,) * 5,
            scratch_shapes=[
                vmem((WIDE, DIM), F32),
                vmem((WIDE, 2 * DIM), BF16),
                vmem((WIDE, DIM), BF16),
                vmem((WIDE, DIM), BF16),
                vmem((28, LEAF, LEAF), BF16),
                vmem((28, LEAF, LEAF), BF16),
                vmem((CLS, WIDE), F32),
                vmem((CLS, WIDE), F32),
                vmem((CLS, LV * LEAF), F32),
                vmem((2 * CLS, WIDE), BF16),
                vmem((LV, LEAF, SKEL), F32),
                vmem((9, 2, SKEL, SKEL), F32),
                vmem((9, 8, SKEL), F32),
                vmem((9, 8, SKEL), I32),
                vmem((LV, SKEL), I32),
                vmem((128, SKEL), F32),
                vmem((SKEL, 128), I32),
                vmem((14, SKEL, SKEL), BF16),
                vmem((14, SKEL, SKEL), BF16),
                vmem((2, SKEL, DIM), F32),
                vmem((3, 4, SKEL, DIM), F32),
                vmem((2, 2, CLS, SKEL), F32),
                vmem((6, 4, HALF, SKEL), F32),
                vmem((2, CLS, SKEL), F32),
                vmem((3, 2, CLS, 128), F32),
                vmem((9, 4, CLS, 128), F32),
                vmem((CLS, 128), F32),
                pltpu.SemaphoreType.DMA((28,)),
                pltpu.SemaphoreType.DMA((72,)),
                pltpu.SemaphoreType.DMA((72,)),
            ],
            compiler_params=pltpu.CompilerParams(
                collective_id=0, has_side_effects=True, vmem_limit_bytes=67043328
            ),
        )(points, right_side, neighbours, leaf_interp, leaf_skeleton, node_skeleton, node_gain, transfer)
        return pl.pallas_call(
            finish,
            out_shape=(out, out),
            in_specs=[any_space] * 5,
            out_specs=(any_space, any_space),
            scratch_shapes=[vmem((CLS, 128), F32)]
            + [vmem((CLS, LV * LEAF), F32)] * 2
            + [vmem((2 * CLS, LV * LEAF), BF16), vmem((CLS, LV * LEAF), F32)]
            + [pltpu.SemaphoreType.DMA((2 * LV + 1,)), pltpu.SemaphoreType.DMA((LV,))],
        )(coef, x0, r1, direction, image)

    in_specs = (
        P("leaf", None), P(None, "leaf"), P("leaf", None), P("leaf", None, None),
        P("leaf", None), P(), P(), P(),
    )
    out_specs = (P(None, "leaf"), P(None, "leaf"))
    return jax.shard_map(device, mesh=mesh, in_specs=in_specs, out_specs=out_specs, check_vma=False)
```
